32 devices in a mesh: sub: 8 (over z, y), dom: 4 (over x, core).
Axes of the slice: x: 2, y: 2, z: 4, core: 2. Of those that a mesh axis runs over, the one named last changes fastest.
Arguments:
- source_points: float32 [128, 3, 4096], P(('sub', 'dom')), may hold values from -4 to 4
- boundary: float32 [128, 8, 6, 128], P(('sub', 'dom')), may hold values from -4 to 4, as said below
- poses: float32 [12, 128], replicated, may hold values from -2 to 2, as said below
- anchor: float32 [128], P(('sub', 'dom')), may hold values from 0.3 to 3
- edge_target: int32 [128, 4], P(('sub', 'dom')), may hold values from 0 to 47, as said below
- corr_tile: int32 [128, 4, 4], P(('sub', 'dom')), may hold values from 0 to 7
- corr_source: int32 [128, 4, 4, 128], P(('sub', 'dom')), may hold values from 0 to 4095
- corr_lane: int32 [128, 4, 4, 128], P(('sub', 'dom')), may hold values from 0 to 127
Outputs:
- refined_pose: float32 [12, 128], P(None, ('sub', 'dom'))
The draws below stay inside these ranges and needn't reach their ends.
Inputs may be any that keep to these rules, and one draw needn't show every extreme that they name: `poses`: each column holds a rotation matrix, row-major, followed by a translation. `boundary`: in every column of 6 entries the last 3 form a unit vector. `edge_target`: entry v of scan s names scan v % 16 of the previous (v // 16 = 0), the same (1) or the next (2) submap along the closed chain of submaps; it never names s itself; one scan may be named by several edges of s.
All inputs are finite; a program needn't handle non-finite values.
Results may differ from the reference program's by a relative error of at most 0.0001.
Values sent between devices are 32-bit elements; how exact they have to be, the bound alone decides.
No kernel may reach another device: no remote copies, remote signals or barrier semaphores. Data moves between devices by JAX's collectives and lax.ppermute only.
A program may use at most 64 MiB of HBM per device.

```python
import math
import jax
import jax.numpy as jnp
from jax import lax

PTS = 4096
BND = 8
EDGES = 4
CT = 4
CG_ITERS = 2
GN_ITERS = 2
SCAN_SUB = 16
SCANS = 128
N_SUB = 8


def cayley_drawn(vector):
    first, second, third = (vector[0], vector[1], vector[2])
    length_sq = first * first + second * second + third * third
    inverse = 1.0 / (1.0 + length_sq)
    trace_part = 1.0 - length_sq
    entries = [[trace_part + 2.0 * first * first, 2.0 * first * second - 2.0 * third, 2.0 * first * third + 2.0 * second], [2.0 * first * second + 2.0 * third, trace_part + 2.0 * second * second, 2.0 * second * third - 2.0 * first], [2.0 * first * third - 2.0 * second, 2.0 * second * third + 2.0 * first, trace_part + 2.0 * third * third]]
    return jnp.stack([jnp.stack(line) for line in entries]) * inverse


def draw_poses(key, part):
    key_turn, key_move = jax.random.split(jax.random.fold_in(key, 11), 2)
    growth = 0.5 + 1.5 * jnp.arange(SCANS, dtype=jnp.float32) / max(SCANS - 1, 1)
    turning = jax.random.uniform(key_turn, (3, SCANS), jnp.float32, -0.4, 0.4)
    moving = growth * jax.random.uniform(key_move, (3, SCANS), jnp.float32, -1.0, 1.0)
    rotation = cayley_drawn(turning).reshape(9, SCANS)
    return jnp.concatenate([rotation, moving], axis=0).astype(jnp.float32)


def draw_boundary(key, part):
    key_coord, key_height, key_angle = jax.random.split(jax.random.fold_in(key, 23), 3)
    coords = jnp.clip(jax.random.normal(key_coord, (SCANS, BND, 3, 128), jnp.float32), -4.0, 4.0)
    height = jax.random.uniform(key_height, (SCANS, BND, 128), jnp.float32, -1.0, 1.0)
    azimuth = jax.random.uniform(key_angle, (SCANS, BND, 128), jnp.float32, -jnp.pi, jnp.pi)
    radius = jnp.sqrt(jnp.maximum(1.0 - height * height, 0.0))
    normal = jnp.stack([radius * jnp.cos(azimuth), radius * jnp.sin(azimuth), height], axis=2)
    return jnp.concatenate([coords, normal], axis=2).astype(jnp.float32)


def draw_edge_target(key, part):
    own_slot = SCAN_SUB + jnp.arange(SCANS, dtype=jnp.int32) % SCAN_SUB
    raw_pick = jax.random.randint(jax.random.fold_in(key, 37), (SCANS, EDGES), 0, 3 * SCAN_SUB - 1, dtype=jnp.int32)
    return raw_pick + (raw_pick >= own_slot[:, None]).astype(jnp.int32)


def place_ends(array, rng, low, top_value):
    longest = array.shape.index(max(array.shape))
    spots = []
    for shift in (0, 1):
        where = [jax.random.randint(jax.random.fold_in(rng, axis), (), 0, length) for axis, length in enumerate(array.shape)]
        where[longest] = (where[longest] + shift) % array.shape[longest]
        spots.append(tuple(where))
    return array.at[spots[0]].set(low).at[spots[1]].set(top_value)


def shard_levels(own_key, shape, cuts, smallest, high):
    gain, own = 1.0, jax.random.fold_in(own_key, 6)
    for dim, shards_of in cuts:
        draws = jnp.exp(jax.random.uniform(jax.random.fold_in(own, dim), (shards_of,), jnp.float32, smallest / len(cuts), high / len(cuts)))
        gain = gain * jnp.repeat(draws, shape[dim] // shards_of).reshape([-1 if axis == dim else 1 for axis in range(len(shape))])
    return gain


def bell_draw(key, dims, scale, reach, pieces=(), kind=jnp.bfloat16):
    array = scale * jax.random.normal(key, dims, jnp.float32)
    if pieces:
        array = array * shard_levels(key, dims, pieces, -0.22, 0.18)
    return jnp.clip(array, -reach, reach).astype(kind)


def setup_inputs(seed: int = 0) -> dict:
    key_list = jax.random.split(jax.random.key(seed), 9)
    return {
        "source_points": bell_draw(key_list[0], (SCANS, 3, PTS), 1.0, 4.0, ((0, 32),), jnp.float32),
        "boundary": draw_boundary(jax.random.fold_in(key_list[8], 71), 0),
        "poses": draw_poses(jax.random.fold_in(key_list[8], 71), 0),
        "anchor": jnp.clip(jnp.exp(math.log(3.0) - 2.3025851 * jax.random.uniform(key_list[3], (SCANS,), jnp.float32) ** shard_levels(key_list[3], (SCANS,), ((0, 32),), -0.2, 0.2)), 0.3, 3.0),
        "edge_target": draw_edge_target(jax.random.fold_in(key_list[8], 71), 0),
        "corr_tile": place_ends(jax.random.randint(key_list[5], (SCANS, EDGES, CT), 0, BND), jax.random.fold_in(key_list[5], 1), 0, BND - 1).astype(jnp.int32),
        "corr_source": place_ends(jax.random.randint(key_list[6], (SCANS, EDGES, CT, 128), 0, PTS), jax.random.fold_in(key_list[6], 1), 0, PTS - 1).astype(jnp.int32),
        "corr_lane": place_ends(jax.random.randint(key_list[7], (SCANS, EDGES, CT, 128), 0, 128), jax.random.fold_in(key_list[7], 1), 0, 127).astype(jnp.int32),
    }


FINEST = lax.Precision.HIGHEST


def cayley(vector):
    first, second, third = vector[0], vector[1], vector[2]
    length_sq = first * first + second * second + third * third
    inverse = 1.0 / (1.0 + length_sq)
    trace_part = 1.0 - length_sq
    entries = [[trace_part + 2.0 * first * first, 2.0 * first * second - 2.0 * third, 2.0 * first * third + 2.0 * second],
               [2.0 * first * second + 2.0 * third, trace_part + 2.0 * second * second, 2.0 * second * third - 2.0 * first],
               [2.0 * first * third - 2.0 * second, 2.0 * second * third + 2.0 * first, trace_part + 2.0 * third * third]]
    return jnp.stack([jnp.stack(line) for line in entries]) * inverse


def rotate(matrix, vector):
    return jnp.stack([matrix[row_id, 0] * vector[0] + matrix[row_id, 1] * vector[1] + matrix[row_id, 2] * vector[2] for row_id in range(3)])


def update(pose, increment):
    rotation = pose[:9].reshape(3, 3, -1)
    turn_mat = cayley(0.5 * increment[:3])
    rotated = jnp.stack([jnp.stack([turn_mat[row_id, 0] * rotation[0, col_id] + turn_mat[row_id, 1] * rotation[1, col_id] + turn_mat[row_id, 2] * rotation[2, col_id] for col_id in range(3)]) for row_id in range(3)])
    moved_to = rotate(turn_mat, pose[9:]) + increment[3:]
    return jnp.concatenate([rotated.reshape(9, -1), moved_to], axis=0)


def scan_terms(points, pose_here, target_tiles, target_pose, sources, lane_ids):
    edge_count = sources.shape[0]
    picked = jnp.take(points, sources, axis=1)
    placed = rotate(pose_here[:9].reshape(3, 3), picked) + pose_here[9:, None, None, None]
    spread_lanes = jnp.broadcast_to(lane_ids[:, :, None, :], target_tiles.shape)
    chosen = jnp.take_along_axis(target_tiles, spread_lanes, axis=3)
    rotation = target_pose[:9].reshape(3, 3, edge_count)[:, :, :, None, None]
    shifted = target_pose[9:, :, None, None]
    target = rotate(rotation, jnp.stack([chosen[:, :, 0], chosen[:, :, 1], chosen[:, :, 2]])) + shifted
    normal = rotate(rotation, jnp.stack([chosen[:, :, 3], chosen[:, :, 4], chosen[:, :, 5]]))
    offset = target - placed
    misfit = normal[0] * offset[0] + normal[1] * offset[1] + normal[2] * offset[2]
    turned = jnp.stack([placed[1] * normal[2] - placed[2] * normal[1],
                        placed[2] * normal[0] - placed[0] * normal[2],
                        placed[0] * normal[1] - placed[1] * normal[0]])
    jacobian = jnp.concatenate([turned, normal], axis=0).reshape(6, edge_count, -1)
    samples = jacobian.shape[2]
    blocks = jnp.einsum("aem,bem->eab", jacobian, jacobian, precision=FINEST) / samples
    slopes = jnp.einsum("aem,em->ea", jacobian, misfit.reshape(edge_count, -1), precision=FINEST) / samples
    return blocks, slopes


def neighbours(edge_target):
    scan_ids = jnp.arange(SCANS, dtype=jnp.int32)
    submap = scan_ids // SCAN_SUB
    slot_ids = edge_target // SCAN_SUB
    return ((submap[:, None] + slot_ids - 1) % N_SUB) * SCAN_SUB + edge_target % SCAN_SUB


def reference(source_points, boundary, poses, anchor, edge_target, corr_tile, corr_source, corr_lane):
    far_end = neighbours(edge_target).astype(jnp.int32)
    source = jnp.broadcast_to(jnp.arange(SCANS, dtype=jnp.int32)[:, None], far_end.shape)
    from_end = source.reshape(-1)
    to_end = far_end.reshape(-1)
    current = poses
    for turn_id in range(GN_ITERS):
        def per_scan(per_item, current=current):
            points, pose_here, targets, tile_ids, sources, lane_ids = per_item
            return scan_terms(points, pose_here, boundary[targets[:, None], tile_ids], jnp.take(current, targets, axis=1), sources, lane_ids)

        blocks, slopes = lax.map(per_scan, (source_points, current.T, far_end, corr_tile, corr_source, corr_lane))
        blocks = blocks.reshape(-1, 6, 6)
        slopes = slopes.reshape(-1, 6)
        diag_terms = jnp.diagonal(blocks, axis1=1, axis2=2)
        empty = jnp.zeros((6, SCANS), jnp.float32)
        right_side = empty.at[:, from_end].add(slopes.T).at[:, to_end].add(-slopes.T)
        diagonal_sum = anchor[None, :] + empty.at[:, from_end].add(diag_terms.T).at[:, to_end].add(diag_terms.T)

        def apply_system(vector):
            spread = vector[:, from_end] - vector[:, to_end]
            pushed = jnp.einsum("kab,bk->ak", blocks, spread, precision=FINEST)
            return anchor[None, :] * vector + jnp.zeros_like(vector).at[:, from_end].add(pushed).at[:, to_end].add(-pushed)

        residual = right_side
        scaled = residual / diagonal_sum
        direction = scaled
        energy = jnp.sum(residual * scaled)
        increment = jnp.zeros((6, SCANS), jnp.float32)
        for sweep in range(CG_ITERS):
            image = apply_system(direction)
            step_len = energy / jnp.sum(direction * image)
            increment = increment + step_len * direction
            residual = residual - step_len * image
            if sweep + 1 < CG_ITERS:
                scaled = residual / diagonal_sum
                renewed = jnp.sum(residual * scaled)
                direction = scaled + (renewed / energy) * direction
                energy = renewed
        current = update(current, increment)
    return current
```

```python
import functools

import jax
import jax.numpy as jnp
from jax import lax
from jax.experimental import pallas as pl
from jax.experimental.pallas import tpu as pltpu
from jax.sharding import PartitionSpec as P

CG_ITERS = 2
GN_ITERS = 2
LANES = 128
ROWS = 8
AXES = ("sub", "dom")

SYM3 = [(0, 0), (0, 1), (0, 2), (1, 1), (1, 2), (2, 2)]
SYM4 = [(a, b) for a in range(4) for b in range(a, 4)]
N_MOMENTS = len(SYM4) * len(SYM3) + 4 * 3


def at3(a, b):
    return SYM3.index((min(a, b), max(a, b)))


def at4(a, b):
    return SYM4.index((min(a, b), max(a, b)))


def vmem():
    return pl.BlockSpec(memory_space=pltpu.VMEM)


def smem():
    return pl.BlockSpec(memory_space=pltpu.SMEM)


def pack_body(boundary_ref, out_ref):
    count = out_ref.shape[0]
    part = [boundary_ref[:, :, c, :].reshape(count, LANES) for c in range(6)]
    for c in range(3):
        out_ref[:, c, :] = part[3 + c]
    out_ref[:, 3, :] = part[0] * part[3] + part[1] * part[4] + part[2] * part[5]


def pick_body(points_ref, index_ref, out_ref):
    scans, edges, tiles, _ = index_ref.shape
    per_scan = edges * tiles // ROWS
    edges_here = edges // per_scan
    groups = points_ref.shape[2] // LANES
    for s in range(scans):
        for v in range(per_scan):
            index = index_ref[s, v * edges_here : (v + 1) * edges_here].reshape(ROWS, LANES)
            group = index // LANES
            lane = index % LANES
            found = [jnp.zeros((ROWS, LANES), jnp.float32) for _ in range(3)]
            for g in range(groups):
                here = group == g
                for c in range(3):
                    row = points_ref[s, c : c + 1, g * LANES : (g + 1) * LANES]
                    table = jnp.broadcast_to(row, (ROWS, LANES))
                    found[c] = jnp.where(
                        here, jnp.take_along_axis(table, lane, axis=1), found[c]
                    )
            for c in range(3):
                out_ref[c, s * per_scan + v] = found[c]


def moment_body(
    target_ref, tile_ref, anchor_ref, points_ref, lane_ref, window_ref, out_ref, table_ref
):
    scans, edges, tiles, _ = lane_ref.shape
    bnd = window_ref.shape[0] // (3 * scans * lax.axis_size("dom"))
    per_scan = edges * tiles // ROWS
    edges_here = edges // per_scan
    lane_groups = out_ref.shape[1]
    for s in range(scans):
        for j in range(edges):
            for c in range(tiles):
                row = j * tiles + c
                which = target_ref[s, j] * bnd + tile_ref[s, j, c]
                table_ref[s * per_scan + row // ROWS, :, row % ROWS, :] = window_ref[which]
    lane_at = lax.broadcasted_iota(jnp.int32, (ROWS, LANES), 1)
    row_at = lax.broadcasted_iota(jnp.int32, (ROWS, LANES), 0)
    scale = 1.0 / (tiles * LANES)
    lines = [[] for _ in range(lane_groups)]
    for s in range(scans):
        gathered = [jnp.zeros((ROWS, LANES), jnp.float32) for _ in range(lane_groups)]
        for v in range(per_scan):
            at = s * per_scan + v
            lanes = lane_ref[s, v * edges_here : (v + 1) * edges_here].reshape(ROWS, LANES)
            got = [jnp.take_along_axis(table_ref[at, c], lanes, axis=1) for c in range(4)]
            point = [points_ref[c, at] for c in range(3)] + [None]
            pairs = [got[a] * got[b] for a, b in SYM3]
            weighted = [got[a] * got[3] for a in range(3)]
            place = lane_at - (v * edges_here + row_at // tiles)
            slot = 0
            for a, b in SYM4:
                if a == 3:
                    factor = None
                elif b == 3:
                    factor = point[a]
                else:
                    factor = point[a] * point[b]
                for pair in pairs:
                    value = pair if factor is None else factor * pair
                    total = jnp.sum(value, axis=1, keepdims=True)
                    g, off = divmod(slot * edges, LANES)
                    gathered[g] = jnp.where(place == off, total, gathered[g])
                    slot += 1
            for a in range(4):
                for c in range(3):
                    value = weighted[c] if a == 3 else point[a] * weighted[c]
                    total = jnp.sum(value, axis=1, keepdims=True)
                    g, off = divmod(slot * edges, LANES)
                    gathered[g] = jnp.where(place == off, total, gathered[g])
                    slot += 1
        flat = [jnp.sum(part, axis=0, keepdims=True) * scale for part in gathered]
        lane_row = lax.broadcasted_iota(jnp.int32, (1, LANES), 1)
        for j in range(edges):
            g, off = divmod(N_MOMENTS * edges + j, LANES)
            flat[g] = jnp.where(lane_row == off, target_ref[s, j].astype(jnp.float32), flat[g])
        g, off = divmod((N_MOMENTS + 1) * edges, LANES)
        flat[g] = jnp.where(lane_row == off, anchor_ref[s], flat[g])
        for g in range(lane_groups):
            lines[g].append(flat[g])
    for g in range(lane_groups):
        block = jnp.concatenate(lines[g], axis=0)
        for d in range(out_ref.shape[0]):
            out_ref[d, g] = block


def rotate_sym(matrix, moments):
    half = [
        [sum_of(matrix[a][m] * moments[at3(m, k)] for m in range(3)) for k in range(3)]
        for a in range(3)
    ]
    return [sum_of(half[a][k] * matrix[b][k] for k in range(3)) for a, b in SYM3]


def sum_of(terms):
    total = None
    for term in terms:
        total = term if total is None else total + term
    return total


def edge_terms(moments, own, far):
    place = [[own[3 * a + k] for k in range(3)] + [own[9 + a]] for a in range(3)]
    turn = [[far[3 * a + m] for m in range(3)] for a in range(3)]
    shift = far[9:12]
    turned = [
        rotate_sym(turn, moments[len(SYM3) * k : len(SYM3) * (k + 1)]) for k in range(len(SYM4))
    ]
    nn = turned[at4(3, 3)]
    pnn = []
    ppnn = []
    for e in range(len(SYM3)):
        half = [
            [
                sum_of(place[a][k] * turned[at4(k, l)][e] for k in range(4))
                for l in range(4)
            ]
            for a in range(3)
        ]
        pnn.append([half[a][3] for a in range(3)])
        ppnn.append([sum_of(half[a][l] * place[b][l] for l in range(4)) for a, b in SYM3])

    def pn(a, c, d):
        return pnn[at3(c, d)][a]

    def pp(a, b, c, d):
        return ppnn[at3(c, d)][at3(a, b)]

    mixed = moments[len(SYM4) * len(SYM3) :]
    wx = [
        [sum_of(turn[c][m] * mixed[3 * k + m] for m in range(3)) for c in range(3)]
        for k in range(4)
    ]
    pw = [[sum_of(place[a][k] * wx[k][c] for k in range(4)) for c in range(3)] for a in range(3)]
    nw = wx[3]
    nxt = [(1, 2), (2, 0), (0, 1)]
    block = [[None] * 6 for _ in range(6)]
    for i, (j, k) in enumerate(nxt):
        for i2, (j2, k2) in enumerate(nxt):
            if i2 >= i:
                block[i][i2] = (
                    pp(j, j2, k, k2) - pp(j, k2, k, j2) - pp(k, j2, j, k2) + pp(k, k2, j, j2)
                )
        for d in range(3):
            block[i][3 + d] = pn(j, k, d) - pn(k, j, d)
    for a, b in SYM3:
        block[3 + a][3 + b] = nn[at3(a, b)]
    for a in range(6):
        for b in range(a):
            block[a][b] = block[b][a]
    slopes = []
    for i, (j, k) in enumerate(nxt):
        value = pw[j][k] - pw[k][j]
        for d in range(3):
            value = value + block[i][3 + d] * shift[d]
            value = value - (pp(j, d, k, d) - pp(k, d, j, d))
        slopes.append(value)
    for i in range(3):
        value = nw[i]
        for d in range(3):
            value = value + nn[at3(i, d)] * shift[d] - pn(d, i, d)
        slopes.append(value)
    return block, slopes


def moved(pose, step):
    first, second, third = (0.5 * step[i] for i in range(3))
    length_sq = first * first + second * second + third * third
    inverse = 1.0 / (1.0 + length_sq)
    trace = 1.0 - length_sq
    turn = [
        [
            trace + 2.0 * first * first,
            2.0 * first * second - 2.0 * third,
            2.0 * first * third + 2.0 * second,
        ],
        [
            2.0 * first * second + 2.0 * third,
            trace + 2.0 * second * second,
            2.0 * second * third - 2.0 * first,
        ],
        [
            2.0 * first * third - 2.0 * second,
            2.0 * second * third + 2.0 * first,
            trace + 2.0 * third * third,
        ],
    ]
    turn = [[entry * inverse for entry in line] for line in turn]
    out = [
        sum_of(turn[a][k] * pose[3 * k + c] for k in range(3)) for a in range(3) for c in range(3)
    ]
    out += [sum_of(turn[a][k] * pose[9 + k] for k in range(3)) + step[3 + a] for a in range(3)]
    return out


def solve_body(first_ref, pose_ref, rows_ref, out_ref, *, edges, scan_sub):
    devices, lane_groups, scan_dev, _ = rows_ref.shape
    scans = devices * scan_dev
    chunks = scans // LANES
    blocks = [rows_ref[:, g].reshape(scans, LANES) for g in range(lane_groups)]
    columns = [part.T for part in blocks]

    def plane(slot, height=edges):
        g, off = divmod(slot * edges, LANES)
        return columns[g][off : off + height]

    def end_of(slots, scan):
        end = (scan // scan_sub) * scan_sub + slots - scan_sub
        end = jnp.where(end < 0, end + scans, end)
        return jnp.where(end >= scans, end - scans, end)

    moments = [plane(k) for k in range(N_MOMENTS)]
    end = end_of(
        plane(N_MOMENTS).astype(jnp.int32), lax.broadcasted_iota(jnp.int32, (edges, scans), 1)
    )
    anchor = plane(N_MOMENTS + 1, 1)
    g, off = divmod(N_MOMENTS * edges, LANES)
    hot = []
    for j in range(edges):
        slots = blocks[g][:, off + j : off + j + 1].astype(jnp.int32)
        down = end_of(slots, lax.broadcasted_iota(jnp.int32, (scans, 1), 0))
        across = lax.broadcasted_iota(jnp.int32, (scans, scans), 1)
        hot.append((down == across).astype(jnp.bfloat16))

    def at_end(line):
        wide = []
        for o in range(chunks):
            index = end[:, o * LANES : (o + 1) * LANES]
            found = None
            for q in range(chunks):
                table = jnp.broadcast_to(line[:, q * LANES : (q + 1) * LANES], (edges, LANES))
                value = jnp.take_along_axis(table, index % LANES, axis=1)
                found = value if found is None else jnp.where(index // LANES == q, value, found)
            wide.append(found)
        return wide[0] if chunks == 1 else jnp.concatenate(wide, axis=1)

    def to_end(planes):
        full = jnp.concatenate(planes, axis=0)
        high = full.astype(jnp.bfloat16)
        rest = full - high.astype(jnp.float32)
        middle = rest.astype(jnp.bfloat16)
        low = (rest - middle.astype(jnp.float32)).astype(jnp.bfloat16)
        pieces = jnp.concatenate([high, middle, low], axis=0)
        count = full.shape[0]
        row = lax.broadcasted_iota(jnp.int32, (count, scans), 0) % edges
        total = jnp.zeros((count, scans), jnp.float32)
        for j in range(edges):
            part = jnp.dot(pieces, hot[j], preferred_element_type=jnp.float32)
            part = part[:count] + part[count : 2 * count] + part[2 * count :]
            total = jnp.where(row == j, part, total)
        return [
            jnp.sum(total[edges * i : edges * (i + 1)], axis=0, keepdims=True)
            for i in range(len(planes))
        ]

    def over_edges(value):
        return jnp.sum(value, axis=0, keepdims=True)

    def stack(lines):
        return jnp.concatenate(lines, axis=0)

    def full_sum(value):
        return jnp.sum(jnp.sum(value, axis=0, keepdims=True), axis=1, keepdims=True)

    pose = [pose_ref[i : i + 1, :] for i in range(12)]
    for _ in range(GN_ITERS):
        block, slopes = edge_terms(moments, pose, [at_end(line) for line in pose])
        diag = [block[a][a] for a in range(6)]
        sums = to_end(slopes + diag)
        residual = stack([over_edges(slopes[a]) - sums[a] for a in range(6)])
        diagonal = stack([over_edges(diag[a]) + sums[6 + a] + anchor for a in range(6)])

        def image_of(vector, block=block):
            lines = [vector[a : a + 1] for a in range(6)]
            spread = [line - at_end(line) for line in lines]
            pushed = [sum_of(block[a][b] * spread[b] for b in range(6)) for a in range(6)]
            back = to_end(pushed)
            return stack(
                [anchor * lines[a] + over_edges(pushed[a]) - back[a] for a in range(6)]
            )

        scaled = residual / diagonal
        direction = scaled
        energy = full_sum(residual * scaled)
        increment = jnp.zeros_like(residual)
        for sweep in range(CG_ITERS):
            image = image_of(direction)
            step = energy / full_sum(direction * image)
            increment = increment + step * direction
            if sweep + 1 < CG_ITERS:
                residual = residual - step * image
                scaled = residual / diagonal
                renewed = full_sum(residual * scaled)
                direction = scaled + (renewed / energy) * direction
                energy = renewed
        pose = moved(pose, [increment[a : a + 1] for a in range(6)])
    final = stack(pose)
    lane_at = lax.broadcasted_iota(jnp.int32, final.shape, 1)
    out_at = lax.broadcasted_iota(jnp.int32, out_ref.shape, 1)
    result = jnp.zeros(out_ref.shape, jnp.float32)
    for s in range(scan_dev):
        column = jnp.sum(
            jnp.where(lane_at == first_ref[0] + s, final, 0.0), axis=1, keepdims=True
        )
        result = jnp.where(out_at == s, column, result)
    out_ref[...] = result


def local(source_points, boundary, poses, anchor, edge_target, corr_tile, corr_source, corr_lane):
    scan_dev, bnd = boundary.shape[:2]
    edges, tiles = corr_tile.shape[1:]
    doms = lax.axis_size("dom")
    subs = lax.axis_size("sub")
    devices = subs * doms
    scan_sub = scan_dev * doms
    vectors = scan_dev * edges * tiles // ROWS
    lane_groups = -(-((N_MOMENTS + 2) * edges) // LANES)

    packed = pl.pallas_call(
        pack_body,
        out_shape=jax.ShapeDtypeStruct((scan_dev * bnd, 4, LANES), jnp.float32),
        in_specs=[vmem()],
        out_specs=vmem(),
        name="pack",
    )(boundary)
    before = lax.ppermute(packed, "sub", [((i - 1) % subs, i) for i in range(subs)])
    beyond = lax.ppermute(packed, "sub", [((i + 1) % subs, i) for i in range(subs)])
    picked = pl.pallas_call(
        pick_body,
        out_shape=jax.ShapeDtypeStruct((3, vectors, ROWS, LANES), jnp.float32),
        in_specs=[vmem(), vmem()],
        out_specs=vmem(),
        name="pick",
    )(source_points, corr_source)
    window = lax.all_gather(jnp.stack([before, packed, beyond]), "dom", axis=1, tiled=True)
    window = window.reshape(3 * scan_sub * bnd, 4, LANES)
    rows = pl.pallas_call(
        moment_body,
        out_shape=jax.ShapeDtypeStruct((devices, lane_groups, scan_dev, LANES), jnp.float32),
        in_specs=[smem(), smem(), smem(), vmem(), vmem(), vmem()],
        out_specs=vmem(),
        scratch_shapes=[pltpu.VMEM((vectors, 4, ROWS, LANES), jnp.float32)],
        name="moments",
    )(edge_target, corr_tile, anchor, picked, corr_lane, window)
    rows = lax.all_to_all(rows, AXES, 0, 0)
    first = (lax.axis_index(AXES) * scan_dev).astype(jnp.int32).reshape(1)
    return pl.pallas_call(
        functools.partial(solve_body, edges=edges, scan_sub=scan_sub),
        out_shape=jax.ShapeDtypeStruct((12, scan_dev), jnp.float32),
        in_specs=[smem(), vmem(), vmem()],
        out_specs=vmem(),
        name="solve",
    )(first, poses, rows)


def solution(mesh):
    in_specs = (
        P(AXES, None, None),
        P(AXES, None, None, None),
        P(),
        P(AXES),
        P(AXES, None),
        P(AXES, None, None),
        P(AXES, None, None, None),
        P(AXES, None, None, None),
    )
    out_specs = P(None, AXES)
    return jax.shard_map(local, mesh=mesh, in_specs=in_specs, out_specs=out_specs, check_vma=False)
```

```python
import functools

import jax
import jax.numpy as jnp
from jax import lax
from jax.experimental import pallas as pl
from jax.experimental.pallas import tpu as pltpu
from jax.sharding import PartitionSpec as P

CG_ITERS = 2
GN_ITERS = 2
LANES = 128
ROWS = 8
AXES = ("sub", "dom")

SYM3 = [(0, 0), (0, 1), (0, 2), (1, 1), (1, 2), (2, 2)]
SYM4 = [(a, b) for a in range(4) for b in range(a, 4)]
N_MOMENTS = len(SYM4) * len(SYM3) + 4 * 3


def at3(a, b):
    return SYM3.index((min(a, b), max(a, b)))


def at4(a, b):
    return SYM4.index((min(a, b), max(a, b)))


def vmem():
    return pl.BlockSpec(memory_space=pltpu.VMEM)


def smem():
    return pl.BlockSpec(memory_space=pltpu.SMEM)


def in_vmem(array):
    return pltpu.with_memory_space_constraint(array, pltpu.VMEM)


def pack_body(boundary_ref, out_ref):
    bnd = boundary_ref.shape[2]
    for s in range(boundary_ref.shape[0]):
        part = [boundary_ref[s, c] for c in range(6)]
        part.append(part[0] * part[3] + part[1] * part[4] + part[2] * part[5])
        for c in range(4):
            out_ref[s * bnd : (s + 1) * bnd, c, :] = part[3 + c]


def pick_body(points_ref, index_ref, out_ref):
    scans, edges, tiles, _ = index_ref.shape
    per_scan = edges * tiles // ROWS
    edges_here = edges // per_scan
    groups = points_ref.shape[2] // LANES
    for s in range(scans):
        for v in range(per_scan):
            index = index_ref[s, v * edges_here : (v + 1) * edges_here].reshape(ROWS, LANES)
            group = index // LANES
            lane = index % LANES
            found = [jnp.zeros((ROWS, LANES), jnp.float32) for _ in range(3)]
            for g in range(groups):
                here = group == g
                for c in range(3):
                    row = points_ref[c, s : s + 1, g * LANES : (g + 1) * LANES]
                    table = jnp.broadcast_to(row, (ROWS, LANES))
                    found[c] = jnp.where(
                        here, jnp.take_along_axis(table, lane, axis=1), found[c]
                    )
            for c in range(3):
                out_ref[c, s * per_scan + v] = found[c]


def moment_body(
    target_ref, tile_ref, anchor_ref, points_ref, lane_ref, window_ref, out_ref, table_ref
):
    scans, edges, tiles, _ = lane_ref.shape
    bnd = window_ref.shape[0] // (3 * scans * lax.axis_size("dom"))
    per_scan = edges * tiles // ROWS
    edges_here = edges // per_scan
    lane_groups = out_ref.shape[1]
    for s in range(scans):
        for j in range(edges):
            for c in range(tiles):
                row = j * tiles + c
                which = target_ref[s, j] * bnd + tile_ref[s, j, c]
                table_ref[s * per_scan + row // ROWS, :, row % ROWS, :] = window_ref[which]
    lane_at = lax.broadcasted_iota(jnp.int32, (ROWS, LANES), 1)
    row_at = lax.broadcasted_iota(jnp.int32, (ROWS, LANES), 0)
    scale = 1.0 / (tiles * LANES)
    lines = [[] for _ in range(lane_groups)]
    for s in range(scans):
        gathered = [jnp.zeros((ROWS, LANES), jnp.float32) for _ in range(lane_groups)]
        for v in range(per_scan):
            at = s * per_scan + v
            lanes = lane_ref[s, v * edges_here : (v + 1) * edges_here].reshape(ROWS, LANES)
            got = [jnp.take_along_axis(table_ref[at, c], lanes, axis=1) for c in range(4)]
            point = [points_ref[c, at] for c in range(3)] + [None]
            pairs = [got[a] * got[b] for a, b in SYM3]
            weighted = [got[a] * got[3] for a in range(3)]
            place = lane_at - (v * edges_here + row_at // tiles)
            slot = 0
            for a, b in SYM4:
                if a == 3:
                    factor = None
                elif b == 3:
                    factor = point[a]
                else:
                    factor = point[a] * point[b]
                for pair in pairs:
                    value = pair if factor is None else factor * pair
                    total = jnp.sum(value, axis=1, keepdims=True)
                    g, off = divmod(slot * edges, LANES)
                    gathered[g] = jnp.where(place == off, total, gathered[g])
                    slot += 1
            for a in range(4):
                for c in range(3):
                    value = weighted[c] if a == 3 else point[a] * weighted[c]
                    total = jnp.sum(value, axis=1, keepdims=True)
                    g, off = divmod(slot * edges, LANES)
                    gathered[g] = jnp.where(place == off, total, gathered[g])
                    slot += 1
        flat = [jnp.sum(part, axis=0, keepdims=True) * scale for part in gathered]
        lane_row = lax.broadcasted_iota(jnp.int32, (1, LANES), 1)
        for j in range(edges):
            g, off = divmod(N_MOMENTS * edges + j, LANES)
            flat[g] = jnp.where(lane_row == off, target_ref[s, j].astype(jnp.float32), flat[g])
        g, off = divmod((N_MOMENTS + 1) * edges, LANES)
        flat[g] = jnp.where(lane_row == off, anchor_ref[s], flat[g])
        for g in range(lane_groups):
            lines[g].append(flat[g])
    for g in range(lane_groups):
        block = jnp.concatenate(lines[g], axis=0)
        for d in range(out_ref.shape[0]):
            out_ref[d, g] = block


def rotate_sym(matrix, moments):
    half = [
        [sum_of(matrix[a][m] * moments[at3(m, k)] for m in range(3)) for k in range(3)]
        for a in range(3)
    ]
    return [sum_of(half[a][k] * matrix[b][k] for k in range(3)) for a, b in SYM3]


def sum_of(terms):
    total = None
    for term in terms:
        total = term if total is None else total + term
    return total


def edge_terms(moments, own, far):
    place = [[own[3 * a + k] for k in range(3)] + [own[9 + a]] for a in range(3)]
    turn = [[far[3 * a + m] for m in range(3)] for a in range(3)]
    shift = far[9:12]
    turned = [
        rotate_sym(turn, moments[len(SYM3) * k : len(SYM3) * (k + 1)]) for k in range(len(SYM4))
    ]
    nn = turned[at4(3, 3)]
    pnn = []
    ppnn = []
    for e in range(len(SYM3)):
        half = [
            [
                sum_of(place[a][k] * turned[at4(k, l)][e] for k in range(4))
                for l in range(4)
            ]
            for a in range(3)
        ]
        pnn.append([half[a][3] for a in range(3)])
        ppnn.append([sum_of(half[a][l] * place[b][l] for l in range(4)) for a, b in SYM3])

    def pn(a, c, d):
        return pnn[at3(c, d)][a]

    def pp(a, b, c, d):
        return ppnn[at3(c, d)][at3(a, b)]

    mixed = moments[len(SYM4) * len(SYM3) :]
    wx = [
        [sum_of(turn[c][m] * mixed[3 * k + m] for m in range(3)) for c in range(3)]
        for k in range(4)
    ]
    pw = [[sum_of(place[a][k] * wx[k][c] for k in range(4)) for c in range(3)] for a in range(3)]
    nw = wx[3]
    nxt = [(1, 2), (2, 0), (0, 1)]
    block = [[None] * 6 for _ in range(6)]
    for i, (j, k) in enumerate(nxt):
        for i2, (j2, k2) in enumerate(nxt):
            if i2 >= i:
                block[i][i2] = (
                    pp(j, j2, k, k2) - pp(j, k2, k, j2) - pp(k, j2, j, k2) + pp(k, k2, j, j2)
                )
        for d in range(3):
            block[i][3 + d] = pn(j, k, d) - pn(k, j, d)
    for a, b in SYM3:
        block[3 + a][3 + b] = nn[at3(a, b)]
    for a in range(6):
        for b in range(a):
            block[a][b] = block[b][a]
    slopes = []
    for i, (j, k) in enumerate(nxt):
        value = pw[j][k] - pw[k][j]
        for d in range(3):
            value = value + block[i][3 + d] * shift[d]
            value = value - (pp(j, d, k, d) - pp(k, d, j, d))
        slopes.append(value)
    for i in range(3):
        value = nw[i]
        for d in range(3):
            value = value + nn[at3(i, d)] * shift[d] - pn(d, i, d)
        slopes.append(value)
    return block, slopes


def moved(pose, step):
    first, second, third = (0.5 * step[i] for i in range(3))
    length_sq = first * first + second * second + third * third
    inverse = 1.0 / (1.0 + length_sq)
    trace = 1.0 - length_sq
    turn = [
        [
            trace + 2.0 * first * first,
            2.0 * first * second - 2.0 * third,
            2.0 * first * third + 2.0 * second,
        ],
        [
            2.0 * first * second + 2.0 * third,
            trace + 2.0 * second * second,
            2.0 * second * third - 2.0 * first,
        ],
        [
            2.0 * first * third - 2.0 * second,
            2.0 * second * third + 2.0 * first,
            trace + 2.0 * third * third,
        ],
    ]
    turn = [[entry * inverse for entry in line] for line in turn]
    out = [
        sum_of(turn[a][k] * pose[3 * k + c] for k in range(3)) for a in range(3) for c in range(3)
    ]
    out += [sum_of(turn[a][k] * pose[9 + k] for k in range(3)) + step[3 + a] for a in range(3)]
    return out


def solve_body(first_ref, pose_ref, rows_ref, out_ref, *, edges, scan_sub):
    devices, lane_groups, scan_dev, _ = rows_ref.shape
    scans = devices * scan_dev
    chunks = scans // LANES
    blocks = [rows_ref[:, g].reshape(scans, LANES) for g in range(lane_groups)]
    columns = [part.T for part in blocks]

    def plane(slot, height=edges):
        g, off = divmod(slot * edges, LANES)
        return columns[g][off : off + height]

    def end_of(slots, scan):
        end = (scan // scan_sub) * scan_sub + slots - scan_sub
        end = jnp.where(end < 0, end + scans, end)
        return jnp.where(end >= scans, end - scans, end)

    moments = [plane(k) for k in range(N_MOMENTS)]
    end = end_of(
        plane(N_MOMENTS).astype(jnp.int32), lax.broadcasted_iota(jnp.int32, (edges, scans), 1)
    )
    anchor = plane(N_MOMENTS + 1, 1)
    g, off = divmod(N_MOMENTS * edges, LANES)
    hot = []
    for j in range(edges):
        slots = blocks[g][:, off + j : off + j + 1].astype(jnp.int32)
        down = end_of(slots, lax.broadcasted_iota(jnp.int32, (scans, 1), 0))
        across = lax.broadcasted_iota(jnp.int32, (scans, scans), 1)
        hot.append((down == across).astype(jnp.bfloat16))

    def at_end(line):
        wide = []
        for o in range(chunks):
            index = end[:, o * LANES : (o + 1) * LANES]
            found = None
            for q in range(chunks):
                table = jnp.broadcast_to(line[:, q * LANES : (q + 1) * LANES], (edges, LANES))
                value = jnp.take_along_axis(table, index % LANES, axis=1)
                found = value if found is None else jnp.where(index // LANES == q, value, found)
            wide.append(found)
        return wide[0] if chunks == 1 else jnp.concatenate(wide, axis=1)

    def to_end(planes):
        full = jnp.concatenate(planes, axis=0)
        high = full.astype(jnp.bfloat16)
        rest = full - high.astype(jnp.float32)
        middle = rest.astype(jnp.bfloat16)
        low = (rest - middle.astype(jnp.float32)).astype(jnp.bfloat16)
        pieces = jnp.concatenate([high, middle, low], axis=0)
        count = full.shape[0]
        row = lax.broadcasted_iota(jnp.int32, (count, scans), 0) % edges
        total = jnp.zeros((count, scans), jnp.float32)
        for j in range(edges):
            part = jnp.dot(pieces, hot[j], preferred_element_type=jnp.float32)
            part = part[:count] + part[count : 2 * count] + part[2 * count :]
            total = jnp.where(row == j, part, total)
        return [
            jnp.sum(total[edges * i : edges * (i + 1)], axis=0, keepdims=True)
            for i in range(len(planes))
        ]

    def over_edges(value):
        return jnp.sum(value, axis=0, keepdims=True)

    def stack(lines):
        return jnp.concatenate(lines, axis=0)

    def full_sum(value):
        return jnp.sum(jnp.sum(value, axis=0, keepdims=True), axis=1, keepdims=True)

    pose = [pose_ref[i : i + 1, :] for i in range(12)]
    for _ in range(GN_ITERS):
        block, slopes = edge_terms(moments, pose, [at_end(line) for line in pose])
        diag = [block[a][a] for a in range(6)]
        sums = to_end(slopes + diag)
        residual = stack([over_edges(slopes[a]) - sums[a] for a in range(6)])
        diagonal = stack([over_edges(diag[a]) + sums[6 + a] + anchor for a in range(6)])

        def image_of(vector, block=block):
            lines = [vector[a : a + 1] for a in range(6)]
            spread = [line - at_end(line) for line in lines]
            pushed = [sum_of(block[a][b] * spread[b] for b in range(6)) for a in range(6)]
            back = to_end(pushed)
            return stack(
                [anchor * lines[a] + over_edges(pushed[a]) - back[a] for a in range(6)]
            )

        scaled = residual / diagonal
        direction = scaled
        energy = full_sum(residual * scaled)
        increment = jnp.zeros_like(residual)
        for sweep in range(CG_ITERS):
            image = image_of(direction)
            step = energy / full_sum(direction * image)
            increment = increment + step * direction
            if sweep + 1 < CG_ITERS:
                residual = residual - step * image
                scaled = residual / diagonal
                renewed = full_sum(residual * scaled)
                direction = scaled + (renewed / energy) * direction
                energy = renewed
        pose = moved(pose, [increment[a : a + 1] for a in range(6)])
    final = stack(pose)
    lane_at = lax.broadcasted_iota(jnp.int32, final.shape, 1)
    out_at = lax.broadcasted_iota(jnp.int32, (12, scan_dev), 1)
    result = jnp.zeros((12, scan_dev), jnp.float32)
    for s in range(scan_dev):
        column = jnp.sum(
            jnp.where(lane_at == first_ref[0] + s, final, 0.0), axis=1, keepdims=True
        )
        result = jnp.where(out_at == s, column, result)
    out_ref[...] = result.T


def local(source_points, boundary, poses, anchor, edge_target, corr_tile, corr_source, corr_lane):
    scan_dev, bnd = boundary.shape[:2]
    edges, tiles = corr_tile.shape[1:]
    doms = lax.axis_size("dom")
    subs = lax.axis_size("sub")
    devices = subs * doms
    scan_sub = scan_dev * doms
    vectors = scan_dev * edges * tiles // ROWS
    lane_groups = -(-((N_MOMENTS + 2) * edges) // LANES)

    packed = pl.pallas_call(
        pack_body,
        out_shape=pltpu.VMEM((scan_dev * bnd, 4, LANES), jnp.float32),
        in_specs=[vmem()],
        out_specs=vmem(),
        name="pack",
    )(boundary.transpose(0, 2, 1, 3))
    before = lax.ppermute(packed, "sub", [((i - 1) % subs, i) for i in range(subs)])
    beyond = lax.ppermute(packed, "sub", [((i + 1) % subs, i) for i in range(subs)])
    picked = pl.pallas_call(
        pick_body,
        out_shape=pltpu.VMEM((3, vectors, ROWS, LANES), jnp.float32),
        in_specs=[vmem(), vmem()],
        out_specs=vmem(),
        name="pick",
    )(source_points.transpose(1, 0, 2), corr_source)
    window = lax.all_gather(jnp.stack([before, packed, beyond]), "dom", axis=1, tiled=True)
    window = window.reshape(3 * scan_sub * bnd, 4, LANES)
    rows = pl.pallas_call(
        moment_body,
        out_shape=pltpu.VMEM((devices, lane_groups, scan_dev, LANES), jnp.float32),
        in_specs=[smem(), smem(), smem(), vmem(), vmem(), vmem()],
        out_specs=vmem(),
        scratch_shapes=[pltpu.VMEM((vectors, 4, ROWS, LANES), jnp.float32)],
        name="moments",
    )(edge_target, corr_tile, anchor, in_vmem(picked), corr_lane, in_vmem(window))
    rows = lax.all_to_all(rows, AXES, 0, 0)
    first = (lax.axis_index(AXES) * scan_dev).astype(jnp.int32).reshape(1)
    return pl.pallas_call(
        functools.partial(solve_body, edges=edges, scan_sub=scan_sub),
        out_shape=jax.ShapeDtypeStruct((scan_dev, 12), jnp.float32),
        in_specs=[smem(), vmem(), vmem()],
        out_specs=vmem(),
        name="solve",
    )(first, poses, in_vmem(rows)).T


def solution(mesh):
    in_specs = (
        P(AXES, None, None),
        P(AXES, None, None, None),
        P(),
        P(AXES),
        P(AXES, None),
        P(AXES, None, None),
        P(AXES, None, None, None),
        P(AXES, None, None, None),
    )
    out_specs = P(None, AXES)
    return jax.shard_map(local, mesh=mesh, in_specs=in_specs, out_specs=out_specs, check_vma=False)
```

```python
import functools

import jax
import jax.numpy as jnp
from jax import lax
from jax.experimental import pallas as pl
from jax.experimental.pallas import tpu as pltpu
from jax.sharding import PartitionSpec as P

CG_ITERS = 2
GN_ITERS = 2
LANES = 128
LANE_BITS = 7
ROWS = 8
AXES = ("sub", "dom")

SYM3 = [(0, 0), (0, 1), (0, 2), (1, 1), (1, 2), (2, 2)]
SYM4 = [(a, b) for a in range(4) for b in range(a, 4)]


def at3(a, b):
    return SYM3.index((min(a, b), max(a, b)))


def at4(a, b):
    return SYM4.index((min(a, b), max(a, b)))


def vmem():
    return pl.BlockSpec(memory_space=pltpu.VMEM)


def smem():
    return pl.BlockSpec(memory_space=pltpu.SMEM)


def in_vmem(array):
    return pltpu.with_memory_space_constraint(array, pltpu.VMEM)


def pack_body(boundary_ref, out_ref):
    bnd = boundary_ref.shape[2]
    for s in range(boundary_ref.shape[0]):
        part = [boundary_ref[s, c] for c in range(6)]
        part.append(part[0] * part[3] + part[1] * part[4] + part[2] * part[5])
        for c in range(4):
            out_ref[s * bnd : (s + 1) * bnd, c, :] = part[3 + c]


def pick_body(points_ref, index_ref, out_ref, table_ref, rows_ref):
    scans, edges, tiles, _ = index_ref.shape
    pack = ROWS // edges
    groups = points_ref.shape[2] // LANES
    row_at = lax.broadcasted_iota(jnp.int32, (ROWS, LANES), 0)
    for s in range(scans):
        for c in range(tiles):
            at = (s // pack) * tiles + c
            rows_ref[at, (s % pack) * edges : (s % pack + 1) * edges] = index_ref[s, :, c, :]
    for p in range(scans // pack):
        for g in range(groups):
            for k in range(3):
                table = None
                for n in range(pack):
                    s = p * pack + n
                    row = points_ref[k, s : s + 1, g * LANES : (g + 1) * LANES]
                    wide = jnp.broadcast_to(row, (ROWS, LANES))
                    table = wide if n == 0 else jnp.where(row_at >= n * edges, wide, table)
                table_ref[p, g * 3 + k] = table
    for p in range(scans // pack):
        for c in range(tiles):
            index = rows_ref[p * tiles + c]
            group = lax.shift_right_logical(index, LANE_BITS)
            lane = index & (LANES - 1)
            found = [jnp.zeros((ROWS, LANES), jnp.float32)] * 3
            for g in range(groups):
                here = group == g
                for k in range(3):
                    value = jnp.take_along_axis(table_ref[p, g * 3 + k], lane, axis=1)
                    found[k] = jnp.where(here, value, found[k])
            for k in range(3):
                out_ref[k, p * tiles + c] = found[k]


def moment_slot(a, e):
    return a * len(SYM3) + e


def mixed_slot(a, c):
    return len(SYM4) * len(SYM3) + 4 * a + c


END_SLOT = mixed_slot(4, 0)
ANCHOR_SLOT = END_SLOT + 2
N_SLOTS = ANCHOR_SLOT + 1


def moment_body(
    target_ref,
    tile_ref,
    anchor_ref,
    points_ref,
    lane_ref,
    window_ref,
    out_ref,
    table_ref,
    rows_ref,
):
    scans, edges, tiles, _ = lane_ref.shape
    bnd = window_ref.shape[0] // (3 * scans * lax.axis_size("dom"))
    pack = ROWS // edges
    lane_groups = out_ref.shape[1]
    for s in range(scans):
        for j in range(edges):
            for c in range(tiles):
                at = (s // pack) * tiles + c
                if j == 0:
                    row = (s % pack) * edges
                    rows_ref[at, row : row + edges] = lane_ref[s, :, c, :]
                which = target_ref[s, j] * bnd + tile_ref[s, j, c]
                table_ref[at, :, (s % pack) * edges + j, :] = window_ref[which]
    place = lax.broadcasted_iota(jnp.int32, (ROWS, LANES), 1) - (
        lax.broadcasted_iota(jnp.int32, (ROWS, LANES), 0) % edges
    )
    lane_row = lax.broadcasted_iota(jnp.int32, (1, LANES), 1)
    scale = 1.0 / (tiles * LANES)
    lines = [[] for _ in range(lane_groups)]
    for p in range(scans // pack):
        gathered = [jnp.zeros((ROWS, LANES), jnp.float32) for _ in range(lane_groups)]
        sums = {}

        def collect(slot, value, sums=sums):
            sums[slot] = sums[slot] + value if slot in sums else value

        for c in range(tiles):
            at = p * tiles + c
            lanes = rows_ref[at]
            got = [jnp.take_along_axis(table_ref[at, k], lanes, axis=1) for k in range(4)]
            point = [points_ref[k, at] for k in range(3)]
            pairs = [got[a] * got[b] for a, b in SYM3]
            weighted = [got[a] * got[3] for a in range(3)]
            for q, (a, b) in enumerate(SYM4):
                if a == 3:
                    values = pairs
                else:
                    factor = point[a] if b == 3 else point[a] * point[b]
                    values = [factor * pair for pair in pairs]
                for e, value in enumerate(values):
                    collect(moment_slot(q, e), value)
            for a in range(4):
                for k in range(3):
                    value = weighted[k] if a == 3 else point[a] * weighted[k]
                    collect(mixed_slot(a, k), value)
        for slot, value in sums.items():
            total = jnp.sum(value, axis=1, keepdims=True)
            g, off = divmod(slot * edges, LANES)
            gathered[g] = jnp.where(place == off, total, gathered[g])
        for n in range(pack):
            s = p * pack + n
            flat = [
                jnp.sum(part[n * edges : (n + 1) * edges], axis=0, keepdims=True) * scale
                for part in gathered
            ]
            for j in range(2 * edges):
                g, off = divmod(END_SLOT * edges + j, LANES)
                slot = target_ref[s, j % edges].astype(jnp.float32)
                flat[g] = jnp.where(lane_row == off, slot, flat[g])
            g, off = divmod(ANCHOR_SLOT * edges, LANES)
            flat[g] = jnp.where(lane_row == off, anchor_ref[s], flat[g])
            for g in range(lane_groups):
                lines[g].append(flat[g])
    for g in range(lane_groups):
        block = jnp.concatenate(lines[g], axis=0)
        for d in range(out_ref.shape[0]):
            out_ref[d, g] = block


def sum_of(terms):
    total = None
    for term in terms:
        total = term if total is None else total + term
    return total


def product(left, right):
    return [
        [sum_of(left[a][k] * right[k][b] for k in range(3)) for b in range(3)] for a in range(3)
    ]


def transposed(matrix):
    return [[matrix[b][a] for b in range(3)] for a in range(3)]


def applied(matrix, vector):
    return [sum_of(matrix[a][k] * vector[k] for k in range(3)) for a in range(3)]


def cross(left, right):
    return [
        left[1] * right[2] - left[2] * right[1],
        left[2] * right[0] - left[0] * right[2],
        left[0] * right[1] - left[1] * right[0],
    ]


def rotated_sym(matrix, entries):
    half = product(matrix, [[entries[at3(m, k)] for k in range(3)] for m in range(3)])
    return [sum_of(half[a][k] * matrix[b][k] for k in range(3)) for a, b in SYM3]


NEXT = [(1, 2), (2, 0), (0, 1)]


def edge_terms(pair_of, own, far, swap):
    turn = [[far[3 * a + k] for k in range(3)] for a in range(3)]
    here = [[own[3 * a + k] for k in range(3)] for a in range(3)]
    start = own[9:12]
    back = transposed(turn)
    relative = product(back, here)
    shift = applied(back, [far[9 + a] - start[a] for a in range(3)])

    def halves(vector):
        return [vector, swap(vector)]

    mm = []
    xmm = [[] for _ in range(3)]
    xxmm = [[] for _ in range(6)]
    for e in range(0, len(SYM3), 2):
        moment = [pair_of(moment_slot(q, e)) for q in range(len(SYM4))]
        mm += halves(moment[at4(3, 3)])
        for a, part in enumerate(applied(relative, [moment[at4(k, 3)] for k in range(3)])):
            xmm[a] += halves(part)
        square = rotated_sym(relative, [moment[at4(a, b)] for a, b in SYM3])
        for n, part in enumerate(square):
            xxmm[n] += halves(part)
    mw = []
    xmw = [[] for _ in range(3)]
    for c in (0, 2):
        moment = [pair_of(mixed_slot(a, c)) for a in range(4)]
        mw += halves(moment[3])
        for a, part in enumerate(applied(relative, moment[:3])):
            xmw[a] += halves(part)

    def xm(a, c, d):
        return xmm[a][at3(c, d)]

    def xx(a, b, c, d):
        return xxmm[at3(a, b)][at3(c, d)]

    upper = []
    for i, i2 in SYM3:
        (j, k), (j2, k2) = NEXT[i], NEXT[i2]
        upper.append(xx(j, j2, k, k2) - xx(j, k2, k, j2) - xx(k, j2, j, k2) + xx(k, k2, j, j2))
    mixed = [[xm(j, k, d) - xm(k, j, d) for d in range(3)] for j, k in NEXT]
    lower = mm
    slope_upper = []
    for i, (j, k) in enumerate(NEXT):
        value = xmw[j][k] - xmw[k][j]
        value = value + sum_of(mixed[i][d] * shift[d] for d in range(3))
        slope_upper.append(value - sum_of(xx(j, d, k, d) - xx(k, d, j, d) for d in range(3)))
    slope_lower = []
    for i in range(3):
        value = mw[i] + sum_of(lower[at3(i, d)] * shift[d] for d in range(3))
        slope_lower.append(value - sum_of(xm(d, i, d) for d in range(3)))

    lower = rotated_sym(turn, lower)
    upper = rotated_sym(turn, upper)
    mixed = product(product(turn, mixed), back)
    slope_lower = applied(turn, slope_lower)
    slope_upper = applied(turn, slope_upper)
    slope_upper = [u + v for u, v in zip(slope_upper, cross(start, slope_lower))]
    turned = [cross(start, [lower[at3(k, d)] for k in range(3)]) for d in range(3)]
    moved_mixed = [[mixed[a][d] + turned[d][a] for d in range(3)] for a in range(3)]
    first = [cross(start, mixed[b]) for b in range(3)]
    second = [cross(start, moved_mixed[a]) for a in range(3)]
    block = [[None] * 6 for _ in range(6)]
    for n, (a, b) in enumerate(SYM3):
        block[a][b] = block[b][a] = upper[n] + first[b][a] + second[a][b]
        block[3 + a][3 + b] = block[3 + b][3 + a] = lower[n]
    for a in range(3):
        for d in range(3):
            block[a][3 + d] = block[3 + d][a] = moved_mixed[a][d]
    return block, slope_upper + slope_lower


def moved(pose, step):
    first, second, third = (0.5 * step[i] for i in range(3))
    length_sq = first * first + second * second + third * third
    inverse = 1.0 / (1.0 + length_sq)
    trace = 1.0 - length_sq
    turn = [
        [
            trace + 2.0 * first * first,
            2.0 * first * second - 2.0 * third,
            2.0 * first * third + 2.0 * second,
        ],
        [
            2.0 * first * second + 2.0 * third,
            trace + 2.0 * second * second,
            2.0 * second * third - 2.0 * first,
        ],
        [
            2.0 * first * third - 2.0 * second,
            2.0 * second * third + 2.0 * first,
            trace + 2.0 * third * third,
        ],
    ]
    turn = [[entry * inverse for entry in line] for line in turn]
    out = [
        sum_of(turn[a][k] * pose[3 * k + c] for k in range(3)) for a in range(3) for c in range(3)
    ]
    out += [sum_of(turn[a][k] * pose[9 + k] for k in range(3)) + step[3 + a] for a in range(3)]
    return out


def solve_body(first_ref, pose_ref, rows_ref, out_ref, moment_ref, *, edges, scan_sub):
    devices, lane_groups, scan_dev, _ = rows_ref.shape
    scans = devices * scan_dev
    chunks = scans // LANES
    half = ROWS // 2
    blocks = [rows_ref[:, g].reshape(scans, LANES) for g in range(lane_groups)]
    for g in range(lane_groups):
        moment_ref[g * LANES : (g + 1) * LANES] = blocks[g].T

    def pair_of(slot):
        return moment_ref[slot * edges : slot * edges + ROWS]

    def end_of(slots, scan):
        end = (scan // scan_sub) * scan_sub + slots - scan_sub
        end = jnp.where(end < 0, end + scans, end)
        return jnp.where(end >= scans, end - scans, end)

    end = end_of(
        pair_of(END_SLOT).astype(jnp.int32), lax.broadcasted_iota(jnp.int32, (ROWS, scans), 1)
    )
    anchor = moment_ref[ANCHOR_SLOT * edges : ANCHOR_SLOT * edges + 1]
    g, off = divmod(END_SLOT * edges, LANES)
    minus = []
    plus = []
    for j in range(edges):
        slots = blocks[g][:, off + j : off + j + 1].astype(jnp.int32)
        down = lax.broadcasted_iota(jnp.int32, (scans, scans), 0)
        far = end_of(slots, lax.broadcasted_iota(jnp.int32, (scans, 1), 0))
        across = lax.broadcasted_iota(jnp.int32, (scans, scans), 1)
        here = jnp.where(down == across, 1.0, 0.0)
        there = jnp.where(far == across, 1.0, 0.0)
        minus.append((here - there).astype(jnp.bfloat16))
        plus.append((here + there).astype(jnp.bfloat16))
    minus = jnp.concatenate(minus, axis=0)
    plus = jnp.concatenate(plus, axis=0)
    upper = lax.broadcasted_iota(jnp.int32, (ROWS, scans), 0) < edges

    def swap(vector):
        return jnp.concatenate([vector[half:], vector[:half]], axis=0)

    def wide(line):
        return jnp.broadcast_to(line, (ROWS, scans))

    def at_end(table):
        parts = []
        for o in range(chunks):
            index = end[:, o * LANES : (o + 1) * LANES]
            found = None
            for q in range(chunks):
                value = jnp.take_along_axis(
                    table[:, q * LANES : (q + 1) * LANES], index & (LANES - 1), axis=1
                )
                found = value if found is None else jnp.where(lax.shift_right_logical(index, LANE_BITS) == q, value, found)
            parts.append(found)
        return parts[0] if chunks == 1 else jnp.concatenate(parts, axis=1)

    def to_scans(planes, matrix):
        empty = jnp.zeros((ROWS - len(planes), scans), jnp.float32)
        full = jnp.concatenate(
            [
                jnp.concatenate([plane[j : j + 1] for plane in planes] + [empty], axis=0)
                for j in range(edges)
            ],
            axis=1,
        )
        high = full.astype(jnp.bfloat16).astype(jnp.float32)
        rest = full - high
        middle = rest.astype(jnp.bfloat16).astype(jnp.float32)
        pieces = jnp.concatenate([high, middle, rest - middle], axis=0).astype(jnp.bfloat16)
        out = jnp.dot(pieces, matrix, preferred_element_type=jnp.float32)
        return out[:ROWS] + out[ROWS : 2 * ROWS] + out[2 * ROWS :]

    def full_sum(value):
        return jnp.sum(jnp.sum(value, axis=1, keepdims=True), axis=0, keepdims=True)

    pose = [pose_ref[i : i + 1, :] for i in range(12)]
    for _ in range(GN_ITERS):
        own = [wide(line) for line in pose]
        block, slopes = edge_terms(pair_of, own, [at_end(line) for line in own], swap)
        residual = to_scans(slopes, minus)
        diagonal = to_scans([block[a][a] for a in range(6)], plus) + anchor

        def pushed_by(vector, block=block):
            lines = [wide(vector[a : a + 1]) for a in range(6)]
            spread = [line - at_end(line) for line in lines]
            return spread, [sum_of(block[a][b] * spread[b] for b in range(6)) for a in range(6)]

        scaled = residual / diagonal
        direction = scaled
        energy = full_sum(residual * scaled)
        increment = jnp.zeros_like(residual)
        spread, pushed = pushed_by(direction)
        for sweep in range(CG_ITERS):
            inner = jnp.where(upper, sum_of(spread[a] * pushed[a] for a in range(6)), 0.0)
            step = energy / full_sum(inner + anchor * direction * direction)
            increment = increment + step * direction
            if sweep + 1 < CG_ITERS:
                image = to_scans(pushed, minus) + anchor * direction
                residual = residual - step * image
                scaled = residual / diagonal
                renewed = full_sum(residual * scaled)
                fresh_spread, fresh_pushed = pushed_by(scaled)
                ratio = renewed / energy
                spread = [fresh_spread[a] + ratio * spread[a] for a in range(6)]
                pushed = [fresh_pushed[a] + ratio * pushed[a] for a in range(6)]
                direction = scaled + ratio * direction
                energy = renewed
        pose = moved(pose, [increment[a : a + 1] for a in range(6)])
    final = jnp.concatenate(pose, axis=0)
    lane_at = lax.broadcasted_iota(jnp.int32, final.shape, 1)
    out_at = lax.broadcasted_iota(jnp.int32, (12, scan_dev), 1)
    result = jnp.zeros((12, scan_dev), jnp.float32)
    for s in range(scan_dev):
        column = jnp.sum(
            jnp.where(lane_at == first_ref[0] + s, final, 0.0), axis=1, keepdims=True
        )
        result = jnp.where(out_at == s, column, result)
    out_ref[...] = result.T


def local(source_points, boundary, poses, anchor, edge_target, corr_tile, corr_source, corr_lane):
    scan_dev, bnd = boundary.shape[:2]
    edges, tiles = corr_tile.shape[1:]
    doms = lax.axis_size("dom")
    subs = lax.axis_size("sub")
    devices = subs * doms
    scan_sub = scan_dev * doms
    vectors = scan_dev * edges * tiles // ROWS
    lane_groups = -(-N_SLOTS * edges // LANES)

    packed = pl.pallas_call(
        pack_body,
        out_shape=pltpu.VMEM((scan_dev * bnd, 4, LANES), jnp.float32),
        in_specs=[vmem()],
        out_specs=vmem(),
        name="pack",
    )(boundary.transpose(0, 2, 1, 3))
    before = lax.ppermute(packed, "sub", [((i - 1) % subs, i) for i in range(subs)])
    beyond = lax.ppermute(packed, "sub", [((i + 1) % subs, i) for i in range(subs)])
    picked = pl.pallas_call(
        pick_body,
        out_shape=pltpu.VMEM((3, vectors, ROWS, LANES), jnp.float32),
        in_specs=[vmem(), vmem()],
        out_specs=vmem(),
        scratch_shapes=[
            pltpu.VMEM(
                (scan_dev * edges // ROWS, 3 * source_points.shape[2] // LANES, ROWS, LANES),
                jnp.float32,
            ),
            pltpu.VMEM((vectors, ROWS, LANES), jnp.int32),
        ],
        name="pick",
    )(source_points.transpose(1, 0, 2), corr_source)
    window = lax.all_gather(jnp.stack([before, packed, beyond]), "dom", axis=1, tiled=True)
    window = window.reshape(3 * scan_sub * bnd, 4, LANES)
    rows = pl.pallas_call(
        moment_body,
        out_shape=pltpu.VMEM((devices, lane_groups, scan_dev, LANES), jnp.float32),
        in_specs=[smem(), smem(), smem(), vmem(), vmem(), vmem()],
        out_specs=vmem(),
        scratch_shapes=[
            pltpu.VMEM((vectors, 4, ROWS, LANES), jnp.float32),
            pltpu.VMEM((vectors, ROWS, LANES), jnp.int32),
        ],
        name="moments",
    )(edge_target, corr_tile, anchor, in_vmem(picked), in_vmem(corr_lane), in_vmem(window))
    rows = lax.all_to_all(rows, AXES, 0, 0)
    first = (lax.axis_index(AXES) * scan_dev).astype(jnp.int32).reshape(1)
    return pl.pallas_call(
        functools.partial(solve_body, edges=edges, scan_sub=scan_sub),
        out_shape=jax.ShapeDtypeStruct((scan_dev, 12), jnp.float32),
        in_specs=[smem(), vmem(), vmem()],
        out_specs=vmem(),
        scratch_shapes=[
            pltpu.VMEM((lane_groups * LANES, devices * scan_dev), jnp.float32),
        ],
        name="solve",
    )(first, in_vmem(poses), in_vmem(rows)).T


def solution(mesh):
    in_specs = (
        P(AXES, None, None),
        P(AXES, None, None, None),
        P(),
        P(AXES),
        P(AXES, None),
        P(AXES, None, None),
        P(AXES, None, None, None),
        P(AXES, None, None, None),
    )
    out_specs = P(None, AXES)
    return jax.shard_map(local, mesh=mesh, in_specs=in_specs, out_specs=out_specs, check_vma=False)
```

```python
import functools

import jax
import jax.numpy as jnp
from jax import lax
from jax.experimental import pallas as pl
from jax.experimental.pallas import tpu as pltpu
from jax.sharding import PartitionSpec as P


CG_ITERS = 2
GN_ITERS = 2
LANES = 128
LANE_BITS = 7
ROWS = 8
AXES = ("sub", "dom")

SYM3 = [(0, 0), (0, 1), (0, 2), (1, 1), (1, 2), (2, 2)]
SYM4 = [(a, b) for a in range(4) for b in range(a, 4)]


def at3(a, b):
    return SYM3.index((min(a, b), max(a, b)))


def at4(a, b):
    return SYM4.index((min(a, b), max(a, b)))


def vmem():
    return pl.BlockSpec(memory_space=pltpu.VMEM)


def smem():
    return pl.BlockSpec(memory_space=pltpu.SMEM)


def in_vmem(array):
    return pltpu.with_memory_space_constraint(array, pltpu.VMEM)


def pack_body(boundary_ref, out_ref):
    bnd = boundary_ref.shape[2]
    for s in range(boundary_ref.shape[0]):
        part = [boundary_ref[s, c] for c in range(6)]
        part.append(part[0] * part[3] + part[1] * part[4] + part[2] * part[5])
        for c in range(4):
            out_ref[s * bnd : (s + 1) * bnd, c, :] = part[3 + c]


PIECES = [[0, 2, 1], [4, 6, 5], [8, 3, 9], [10, 7, 11]]


def window_of(packed, subs, doms):
    before = lax.ppermute(packed, "sub", [((i - 1) % subs, i) for i in range(subs)])
    beyond = lax.ppermute(packed, "sub", [((i + 1) % subs, i) for i in range(subs)])
    if doms != len(PIECES):
        window = lax.all_gather(jnp.stack([before, packed, beyond]), "dom", axis=1, tiled=True)
        return window.reshape(-1, *packed.shape[1:])

    def partner(array, distance):
        return lax.ppermute(array, "dom", [(i ^ distance, i) for i in range(doms)])

    own = jnp.concatenate([before, beyond, packed, partner(packed, 2)], axis=0)
    far = partner(own[: 2 * packed.shape[0]], 2)
    near = partner(own, 1)
    return jnp.concatenate([own, near, far, partner(far, 1)], axis=0)


def place_of(target, scans, scan_sub):
    if scan_sub // scans != len(PIECES):
        return target
    slot = lax.div(target, scan_sub)
    inside = lax.rem(target, scan_sub)
    apart = lax.div(inside, scans) ^ lax.axis_index("dom")
    piece = jnp.int32(0)
    for n, line in enumerate(PIECES):
        for k, at in enumerate(line):
            piece = jnp.where((apart == n) & (slot == k), jnp.int32(at), piece)
    return piece * scans + lax.rem(inside, scans)


def pick_body(
    target_ref,
    tile_ref,
    anchor_ref,
    points_ref,
    index_ref,
    lane_ref,
    out_ref,
    lanes_ref,
    which_ref,
    tail_ref,
    table_ref,
    rows_ref,
    *,
    bnd,
):
    scans, edges, tiles, _ = index_ref.shape
    pack = ROWS // edges
    groups = points_ref.shape[2] // LANES
    row_at = lax.broadcasted_iota(jnp.int32, (ROWS, LANES), 0)
    lane_row = lax.broadcasted_iota(jnp.int32, (1, LANES), 1)
    subs = lax.axis_size("sub")
    scan_sub = scans * lax.axis_size("dom")
    for s in range(scans):
        tail = jnp.zeros((1, LANES), jnp.float32)
        for j in range(edges):
            target = target_ref[s, j]
            group = lax.rem(lax.axis_index("sub") + lax.div(target, scan_sub) + subs - 1, subs)
            end = (group * scan_sub + lax.rem(target, scan_sub)).astype(jnp.float32)
            for at in (END_SLOT * edges + j, (END_SLOT + 1) * edges + j):
                tail = jnp.where(lane_row == at % LANES, end, tail)
            first = place_of(target, scans, scan_sub) * bnd
            for c in range(tiles):
                row = (s * edges + j) * tiles + c
                which_ref[row : row + 1] = jnp.full(
                    (1, LANES), first + tile_ref[s, j, c], jnp.int32
                )
        tail_ref[s : s + 1] = jnp.where(
            lane_row == ANCHOR_SLOT * edges % LANES, anchor_ref[s], tail
        )
        for c in range(tiles):
            at = (s // pack) * tiles + c
            own = slice((s % pack) * edges, (s % pack + 1) * edges)
            rows_ref[at, own] = index_ref[s, :, c, :]
            lanes_ref[at, own] = lane_ref[s, :, c, :]
    for p in range(scans // pack):
        for g in range(groups):
            for k in range(3):
                table = None
                for n in range(pack):
                    s = p * pack + n
                    row = points_ref[k, s : s + 1, g * LANES : (g + 1) * LANES]
                    wide = jnp.broadcast_to(row, (ROWS, LANES))
                    table = wide if n == 0 else jnp.where(row_at >= n * edges, wide, table)
                table_ref[p, g * 3 + k] = table
    for p in range(scans // pack):
        for c in range(tiles):
            index = rows_ref[p * tiles + c]
            group = lax.shift_right_logical(index, LANE_BITS)
            lane = index & (LANES - 1)
            found = [jnp.zeros((ROWS, LANES), jnp.float32)] * 3
            for g in range(groups):
                here = group == g
                for k in range(3):
                    value = jnp.take_along_axis(table_ref[p, g * 3 + k], lane, axis=1)
                    found[k] = jnp.where(here, value, found[k])
            for k in range(3):
                out_ref[k, p * tiles + c] = found[k]


def moment_slot(a, e):
    return a * len(SYM3) + e


def mixed_slot(a, c):
    return len(SYM4) * len(SYM3) + 4 * a + c


END_SLOT = mixed_slot(4, 0)
ANCHOR_SLOT = END_SLOT + 2
N_SLOTS = ANCHOR_SLOT + 1


def moment_body(
    which_ref, tail_ref, points_ref, lanes_ref, window_ref, out_ref, table_ref, *, edges, tiles
):
    lane_groups, scans = out_ref.shape[1:3]
    pack = ROWS // edges
    for s in range(scans):
        for j in range(edges):
            for c in range(tiles):
                which = which_ref[(s * edges + j) * tiles + c, 0]
                at = (s // pack) * tiles + c
                table_ref[at, :, (s % pack) * edges + j, :] = window_ref[which]
    place = lax.broadcasted_iota(jnp.int32, (ROWS, LANES), 1) - (
        lax.broadcasted_iota(jnp.int32, (ROWS, LANES), 0) % edges
    )
    scale = 1.0 / (tiles * LANES)
    lines = [[] for _ in range(lane_groups)]
    for p in range(scans // pack):
        gathered = [jnp.zeros((ROWS, LANES), jnp.float32) for _ in range(lane_groups)]
        sums = {}

        def collect(slot, value, sums=sums):
            sums[slot] = sums[slot] + value if slot in sums else value

        for c in range(tiles):
            at = p * tiles + c
            lanes = lanes_ref[at]
            got = [jnp.take_along_axis(table_ref[at, k], lanes, axis=1) for k in range(4)]
            point = [points_ref[k, at] for k in range(3)]
            pairs = [got[a] * got[b] for a, b in SYM3]
            weighted = [got[a] * got[3] for a in range(3)]
            for q, (a, b) in enumerate(SYM4):
                if a == 3:
                    values = pairs
                else:
                    factor = point[a] if b == 3 else point[a] * point[b]
                    values = [factor * pair for pair in pairs]
                for e, value in enumerate(values):
                    collect(moment_slot(q, e), value)
            for a in range(4):
                for k in range(3):
                    value = weighted[k] if a == 3 else point[a] * weighted[k]
                    collect(mixed_slot(a, k), value)
        for slot, value in sums.items():
            total = jnp.sum(value, axis=1, keepdims=True)
            g, off = divmod(slot * edges, LANES)
            gathered[g] = jnp.where(place == off, total, gathered[g])
        for n in range(pack):
            s = p * pack + n
            flat = [
                jnp.sum(part[n * edges : (n + 1) * edges], axis=0, keepdims=True) * scale
                for part in gathered
            ]
            for g in range(lane_groups):
                lines[g].append(flat[g])
    for g in range(lane_groups):
        block = jnp.concatenate(lines[g], axis=0)
        if g == lane_groups - 1:
            block = block + tail_ref[...]
        for d in range(out_ref.shape[0]):
            out_ref[d, g] = block


def sum_of(terms):
    total = None
    for term in terms:
        total = term if total is None else total + term
    return total


def product(left, right):
    return [
        [sum_of(left[a][k] * right[k][b] for k in range(3)) for b in range(3)] for a in range(3)
    ]


def transposed(matrix):
    return [[matrix[b][a] for b in range(3)] for a in range(3)]


def applied(matrix, vector):
    return [sum_of(matrix[a][k] * vector[k] for k in range(3)) for a in range(3)]


def cross(left, right):
    return [
        left[1] * right[2] - left[2] * right[1],
        left[2] * right[0] - left[0] * right[2],
        left[0] * right[1] - left[1] * right[0],
    ]


def rotated_sym(matrix, entries):
    half = product(matrix, [[entries[at3(m, k)] for k in range(3)] for m in range(3)])
    return [sum_of(half[a][k] * matrix[b][k] for k in range(3)) for a, b in SYM3]


NEXT = [(1, 2), (2, 0), (0, 1)]


def edge_terms(pair_of, own, far, swap):
    turn = [[far[3 * a + k] for k in range(3)] for a in range(3)]
    here = [[own[3 * a + k] for k in range(3)] for a in range(3)]
    start = own[9:12]
    back = transposed(turn)
    relative = product(back, here)
    shift = applied(back, [far[9 + a] - start[a] for a in range(3)])

    def halves(vector):
        return [vector, swap(vector)]

    mm = []
    xmm = [[] for _ in range(3)]
    xxmm = [[] for _ in range(6)]
    for e in range(0, len(SYM3), 2):
        moment = [pair_of(moment_slot(q, e)) for q in range(len(SYM4))]
        mm += halves(moment[at4(3, 3)])
        for a, part in enumerate(applied(relative, [moment[at4(k, 3)] for k in range(3)])):
            xmm[a] += halves(part)
        square = rotated_sym(relative, [moment[at4(a, b)] for a, b in SYM3])
        for n, part in enumerate(square):
            xxmm[n] += halves(part)
    mw = []
    xmw = [[] for _ in range(3)]
    for c in (0, 2):
        moment = [pair_of(mixed_slot(a, c)) for a in range(4)]
        mw += halves(moment[3])
        for a, part in enumerate(applied(relative, moment[:3])):
            xmw[a] += halves(part)

    def xm(a, c, d):
        return xmm[a][at3(c, d)]

    def xx(a, b, c, d):
        return xxmm[at3(a, b)][at3(c, d)]

    upper = []
    for i, i2 in SYM3:
        (j, k), (j2, k2) = NEXT[i], NEXT[i2]
        upper.append(xx(j, j2, k, k2) - xx(j, k2, k, j2) - xx(k, j2, j, k2) + xx(k, k2, j, j2))
    mixed = [[xm(j, k, d) - xm(k, j, d) for d in range(3)] for j, k in NEXT]
    lower = mm
    slope_upper = []
    for i, (j, k) in enumerate(NEXT):
        value = xmw[j][k] - xmw[k][j]
        value = value + sum_of(mixed[i][d] * shift[d] for d in range(3))
        slope_upper.append(value - sum_of(xx(j, d, k, d) - xx(k, d, j, d) for d in range(3)))
    slope_lower = []
    for i in range(3):
        value = mw[i] + sum_of(lower[at3(i, d)] * shift[d] for d in range(3))
        slope_lower.append(value - sum_of(xm(d, i, d) for d in range(3)))

    lower = rotated_sym(turn, lower)
    upper = rotated_sym(turn, upper)
    mixed = product(product(turn, mixed), back)
    slope_lower = applied(turn, slope_lower)
    slope_upper = applied(turn, slope_upper)
    slope_upper = [u + v for u, v in zip(slope_upper, cross(start, slope_lower))]
    turned = [cross(start, [lower[at3(k, d)] for k in range(3)]) for d in range(3)]
    moved_mixed = [[mixed[a][d] + turned[d][a] for d in range(3)] for a in range(3)]
    first = [cross(start, mixed[b]) for b in range(3)]
    second = [cross(start, moved_mixed[a]) for a in range(3)]
    block = [[None] * 6 for _ in range(6)]
    for n, (a, b) in enumerate(SYM3):
        block[a][b] = block[b][a] = upper[n] + first[b][a] + second[a][b]
        block[3 + a][3 + b] = block[3 + b][3 + a] = lower[n]
    for a in range(3):
        for d in range(3):
            block[a][3 + d] = block[3 + d][a] = moved_mixed[a][d]
    return block, slope_upper + slope_lower


def moved(pose, step):
    first, second, third = (0.5 * step[i] for i in range(3))
    length_sq = first * first + second * second + third * third
    inverse = 1.0 / (1.0 + length_sq)
    trace = 1.0 - length_sq
    turn = [
        [
            trace + 2.0 * first * first,
            2.0 * first * second - 2.0 * third,
            2.0 * first * third + 2.0 * second,
        ],
        [
            2.0 * first * second + 2.0 * third,
            trace + 2.0 * second * second,
            2.0 * second * third - 2.0 * first,
        ],
        [
            2.0 * first * third - 2.0 * second,
            2.0 * second * third + 2.0 * first,
            trace + 2.0 * third * third,
        ],
    ]
    turn = [[entry * inverse for entry in line] for line in turn]
    out = [
        sum_of(turn[a][k] * pose[3 * k + c] for k in range(3)) for a in range(3) for c in range(3)
    ]
    out += [sum_of(turn[a][k] * pose[9 + k] for k in range(3)) + step[3 + a] for a in range(3)]
    return out


def solve_body(first_ref, pose_ref, rows_ref, out_ref, moment_ref, final_ref, *, edges):
    devices, lane_groups, scan_dev, _ = rows_ref.shape
    scans = devices * scan_dev
    chunks = scans // LANES
    half = ROWS // 2
    blocks = [rows_ref[:, g].reshape(scans, LANES) for g in range(lane_groups)]
    for g in range(lane_groups):
        moment_ref[g * LANES : (g + 1) * LANES] = blocks[g].T

    def pair_of(slot):
        return moment_ref[slot * edges : slot * edges + ROWS]

    end = pair_of(END_SLOT).astype(jnp.int32)
    anchor = moment_ref[ANCHOR_SLOT * edges : ANCHOR_SLOT * edges + 1]
    g, off = divmod(END_SLOT * edges, LANES)
    down = lax.broadcasted_iota(jnp.int32, (scans, scans), 0)
    across = lax.broadcasted_iota(jnp.int32, (scans, scans), 1)
    here = jnp.where(down == across, 1.0, 0.0)
    across = across.astype(jnp.float32)
    minus = []
    plus = []
    for j in range(edges):
        there = jnp.where(blocks[g][:, off + j : off + j + 1] == across, 1.0, 0.0)
        minus.append((here - there).astype(jnp.bfloat16))
        plus.append((here + there).astype(jnp.bfloat16))
    minus = jnp.concatenate(minus, axis=0)
    plus = jnp.concatenate(plus, axis=0)
    upper = lax.broadcasted_iota(jnp.int32, (ROWS, scans), 0) < edges

    def swap(vector):
        return jnp.concatenate([vector[half:], vector[:half]], axis=0)

    def wide(line):
        return jnp.broadcast_to(line, (ROWS, scans))

    def at_end(table):
        parts = []
        for o in range(chunks):
            index = end[:, o * LANES : (o + 1) * LANES]
            found = None
            for q in range(chunks):
                value = jnp.take_along_axis(
                    table[:, q * LANES : (q + 1) * LANES], index & (LANES - 1), axis=1
                )
                found = value if found is None else jnp.where(lax.shift_right_logical(index, LANE_BITS) == q, value, found)
            parts.append(found)
        return parts[0] if chunks == 1 else jnp.concatenate(parts, axis=1)

    def to_scans(planes, matrix):
        empty = jnp.zeros((ROWS - len(planes), scans), jnp.float32)
        full = jnp.concatenate(
            [
                jnp.concatenate([plane[j : j + 1] for plane in planes] + [empty], axis=0)
                for j in range(edges)
            ],
            axis=1,
        )
        high = full.astype(jnp.bfloat16).astype(jnp.float32)
        rest = full - high
        middle = rest.astype(jnp.bfloat16).astype(jnp.float32)
        pieces = jnp.concatenate([high, middle, rest - middle], axis=0).astype(jnp.bfloat16)
        out = jnp.dot(pieces, matrix, preferred_element_type=jnp.float32)
        return out[:ROWS] + out[ROWS : 2 * ROWS] + out[2 * ROWS :]

    def full_sum(value):
        return jnp.sum(jnp.sum(value, axis=1, keepdims=True), axis=0, keepdims=True)

    pose = [pose_ref[i : i + 1, :] for i in range(12)]
    for _ in range(GN_ITERS):
        own = [wide(line) for line in pose]
        block, slopes = edge_terms(pair_of, own, [at_end(line) for line in own], swap)
        residual = to_scans(slopes, minus)
        diagonal = to_scans([block[a][a] for a in range(6)], plus) + anchor

        def pushed_by(vector, block=block):
            lines = [wide(vector[a : a + 1]) for a in range(6)]
            spread = [line - at_end(line) for line in lines]
            return spread, [sum_of(block[a][b] * spread[b] for b in range(6)) for a in range(6)]

        scaled = residual / diagonal
        direction = scaled
        energy = full_sum(residual * scaled)
        increment = jnp.zeros_like(residual)
        spread, pushed = pushed_by(direction)
        for sweep in range(CG_ITERS):
            inner = jnp.where(upper, sum_of(spread[a] * pushed[a] for a in range(6)), 0.0)
            step = energy / full_sum(inner + anchor * direction * direction)
            increment = increment + step * direction
            if sweep + 1 < CG_ITERS:
                image = to_scans(pushed, minus) + anchor * direction
                residual = residual - step * image
                scaled = residual / diagonal
                renewed = full_sum(residual * scaled)
                fresh_spread, fresh_pushed = pushed_by(scaled)
                ratio = renewed / energy
                spread = [fresh_spread[a] + ratio * spread[a] for a in range(6)]
                pushed = [fresh_pushed[a] + ratio * pushed[a] for a in range(6)]
                direction = scaled + ratio * direction
                energy = renewed
        pose = moved(pose, [increment[a : a + 1] for a in range(6)])
    final_ref[...] = jnp.concatenate(pose, axis=0).T
    out_ref[...] = final_ref[pl.ds(pl.multiple_of(first_ref[0], scan_dev), scan_dev)]


def refined(source_points, boundary, poses, anchor, edge_target, corr_tile, corr_source, corr_lane):
    scan_dev, bnd = boundary.shape[:2]
    edges, tiles = corr_tile.shape[1:]
    doms = lax.axis_size("dom")
    subs = lax.axis_size("sub")
    devices = subs * doms
    vectors = scan_dev * edges * tiles // ROWS
    lane_groups = -(-N_SLOTS * edges // LANES)

    packed = pl.pallas_call(
        pack_body,
        out_shape=pltpu.VMEM((scan_dev * bnd, 4, LANES), jnp.float32),
        in_specs=[vmem()],
        out_specs=vmem(),
        name="pack",
    )(in_vmem(boundary.transpose(0, 2, 1, 3)))
    window = window_of(packed, subs, doms)
    assert END_SLOT * edges // LANES == lane_groups - 1
    picked, lanes, which, tail = pl.pallas_call(
        functools.partial(pick_body, bnd=bnd),
        out_shape=[
            pltpu.VMEM((3, vectors, ROWS, LANES), jnp.float32),
            pltpu.VMEM((vectors, ROWS, LANES), jnp.int32),
            pltpu.VMEM((vectors * ROWS, LANES), jnp.int32),
            pltpu.VMEM((scan_dev, LANES), jnp.float32),
        ],
        in_specs=[smem(), smem(), smem(), vmem(), vmem(), vmem()],
        out_specs=[vmem()] * 4,
        scratch_shapes=[
            pltpu.VMEM(
                (scan_dev * edges // ROWS, 3 * source_points.shape[2] // LANES, ROWS, LANES),
                jnp.float32,
            ),
            pltpu.VMEM((vectors, ROWS, LANES), jnp.int32),
        ],
        name="pick",
    )(
        edge_target,
        corr_tile,
        anchor,
        source_points.transpose(1, 0, 2),
        corr_source,
        corr_lane,
    )
    rows = pl.pallas_call(
        functools.partial(moment_body, edges=edges, tiles=tiles),
        out_shape=jax.ShapeDtypeStruct((devices, lane_groups, scan_dev, LANES), jnp.float32),
        in_specs=[vmem()] * 5,
        out_specs=vmem(),
        scratch_shapes=[pltpu.VMEM((vectors, 4, ROWS, LANES), jnp.float32)],
        name="moments",
    )(*(in_vmem(array) for array in [which, tail, picked, lanes, window]))
    rows = lax.all_to_all(rows, AXES, 0, 0)
    first = (lax.axis_index(AXES) * scan_dev).astype(jnp.int32).reshape(1)
    return pl.pallas_call(
        functools.partial(solve_body, edges=edges),
        out_shape=jax.ShapeDtypeStruct((scan_dev, 12), jnp.float32),
        in_specs=[smem(), vmem(), vmem()],
        out_specs=vmem(),
        scratch_shapes=[
            pltpu.VMEM((lane_groups * LANES, devices * scan_dev), jnp.float32),
            pltpu.VMEM((devices * scan_dev, 12), jnp.float32),
        ],
        name="solve",
    )(first, in_vmem(poses), in_vmem(rows)).T


def solution(mesh):
    in_specs = (
        P(AXES, None, None),
        P(AXES, None, None, None),
        P(),
        P(AXES),
        P(AXES, None),
        P(AXES, None, None),
        P(AXES, None, None, None),
        P(AXES, None, None, None),
    )
    out_specs = P(None, AXES)
    step = jax.shard_map(refined, mesh=mesh, in_specs=in_specs, out_specs=out_specs, check_vma=False)
    if mesh.shape["dom"] != len(PIECES):
        return step
    return step
```

```python
import functools

import jax
import jax.numpy as jnp
from jax import lax
from jax.experimental import pallas as pl
from jax.experimental.pallas import tpu as pltpu
from jax.sharding import PartitionSpec as P


CG_ITERS = 2
GN_ITERS = 2
LANES = 128
LANE_BITS = 7
ROWS = 8
AXES = ("sub", "dom")

SYM3 = [(0, 0), (0, 1), (0, 2), (1, 1), (1, 2), (2, 2)]
SYM4 = [(a, b) for a in range(4) for b in range(a, 4)]


def at3(a, b):
    return SYM3.index((min(a, b), max(a, b)))


def at4(a, b):
    return SYM4.index((min(a, b), max(a, b)))


def vmem():
    return pl.BlockSpec(memory_space=pltpu.VMEM)


def smem():
    return pl.BlockSpec(memory_space=pltpu.SMEM)


def in_vmem(array):
    return pltpu.with_memory_space_constraint(array, pltpu.VMEM)


def pack_body(boundary_ref, out_ref):
    bnd = boundary_ref.shape[2]
    for s in range(boundary_ref.shape[0]):
        part = [boundary_ref[s, c] for c in range(6)]
        part.append(part[0] * part[3] + part[1] * part[4] + part[2] * part[5])
        for c in range(4):
            out_ref[s * bnd : (s + 1) * bnd, c, :] = part[3 + c]


PIECES = [[0, 2, 1], [4, 6, 5], [8, 3, 9], [10, 7, 11]]


def window_of(packed, subs, doms):
    before = lax.ppermute(packed, "sub", [((i - 1) % subs, i) for i in range(subs)])
    beyond = lax.ppermute(packed, "sub", [((i + 1) % subs, i) for i in range(subs)])
    if doms != len(PIECES):
        window = lax.all_gather(jnp.stack([before, packed, beyond]), "dom", axis=1, tiled=True)
        return window.reshape(-1, *packed.shape[1:])

    def partner(array, distance):
        return lax.ppermute(array, "dom", [(i ^ distance, i) for i in range(doms)])

    own = jnp.concatenate([before, beyond, packed, partner(packed, 2)], axis=0)
    far_before = partner(before, 2)
    far_beyond = partner(beyond, 2)
    far = jnp.concatenate([far_before, far_beyond], axis=0)
    near = partner(own, 1)
    last = partner(far, 1)
    return jnp.concatenate([own, near, far, last], axis=0)


def place_of(target, scans, scan_sub):
    if scan_sub // scans != len(PIECES):
        return target
    slot = lax.div(target, scan_sub)
    inside = lax.rem(target, scan_sub)
    apart = lax.div(inside, scans) ^ lax.axis_index("dom")
    piece = jnp.int32(0)
    for n, line in enumerate(PIECES):
        for k, at in enumerate(line):
            piece = jnp.where((apart == n) & (slot == k), jnp.int32(at), piece)
    return piece * scans + lax.rem(inside, scans)


def pick_body(
    target_ref,
    tile_ref,
    anchor_ref,
    points_ref,
    index_ref,
    lane_ref,
    out_ref,
    lanes_ref,
    which_ref,
    tail_ref,
    table_ref,
    rows_ref,
    *,
    bnd,
):
    scans, edges, tiles, _ = index_ref.shape
    pack = ROWS // edges
    groups = points_ref.shape[2] // LANES
    row_at = lax.broadcasted_iota(jnp.int32, (ROWS, LANES), 0)
    lane_row = lax.broadcasted_iota(jnp.int32, (1, LANES), 1)
    subs = lax.axis_size("sub")
    scan_sub = scans * lax.axis_size("dom")
    for s in range(scans):
        tail = jnp.zeros((1, LANES), jnp.float32)
        for j in range(edges):
            target = target_ref[s, j]
            group = lax.rem(lax.axis_index("sub") + lax.div(target, scan_sub) + subs - 1, subs)
            end = (group * scan_sub + lax.rem(target, scan_sub)).astype(jnp.float32)
            for at in (END_SLOT * edges + j, (END_SLOT + 1) * edges + j):
                tail = jnp.where(lane_row == at % LANES, end, tail)
            first = place_of(target, scans, scan_sub) * bnd
            for c in range(tiles):
                row = (s * edges + j) * tiles + c
                which_ref[row : row + 1] = jnp.full(
                    (1, LANES), first + tile_ref[s, j, c], jnp.int32
                )
        tail_ref[s : s + 1] = jnp.where(
            lane_row == ANCHOR_SLOT * edges % LANES, anchor_ref[s], tail
        )
        for c in range(tiles):
            at = (s // pack) * tiles + c
            own = slice((s % pack) * edges, (s % pack + 1) * edges)
            rows_ref[at, own] = index_ref[s, :, c, :]
            lanes_ref[at, own] = lane_ref[s, :, c, :]
    for p in range(scans // pack):
        for g in range(groups):
            for k in range(3):
                table = None
                for n in range(pack):
                    s = p * pack + n
                    row = points_ref[k, s : s + 1, g * LANES : (g + 1) * LANES]
                    wide = jnp.broadcast_to(row, (ROWS, LANES))
                    table = wide if n == 0 else jnp.where(row_at >= n * edges, wide, table)
                table_ref[p, g * 3 + k] = table
    for p in range(scans // pack):
        for c in range(tiles):
            index = rows_ref[p * tiles + c]
            group = lax.shift_right_logical(index, LANE_BITS)
            lane = index & (LANES - 1)
            found = [jnp.zeros((ROWS, LANES), jnp.float32)] * 3
            for g in range(groups):
                here = group == g
                for k in range(3):
                    value = jnp.take_along_axis(table_ref[p, g * 3 + k], lane, axis=1)
                    found[k] = jnp.where(here, value, found[k])
            for k in range(3):
                out_ref[k, p * tiles + c] = found[k]


def moment_slot(a, e):
    return a * len(SYM3) + e


def mixed_slot(a, c):
    return len(SYM4) * len(SYM3) + 4 * a + c


END_SLOT = mixed_slot(4, 0)
ANCHOR_SLOT = END_SLOT + 2
N_SLOTS = ANCHOR_SLOT + 1


def moment_body(
    which_ref, tail_ref, points_ref, lanes_ref, window_ref, out_ref, table_ref, *, edges, tiles
):
    lane_groups, scans = out_ref.shape[1:3]
    pack = ROWS // edges
    for s in range(scans):
        for j in range(edges):
            for c in range(tiles):
                which = which_ref[(s * edges + j) * tiles + c, 0]
                at = (s // pack) * tiles + c
                table_ref[at, :, (s % pack) * edges + j, :] = window_ref[which]
    place = lax.broadcasted_iota(jnp.int32, (ROWS, LANES), 1) - (
        lax.broadcasted_iota(jnp.int32, (ROWS, LANES), 0) % edges
    )
    scale = 1.0 / (tiles * LANES)
    lines = [[] for _ in range(lane_groups)]
    for p in range(scans // pack):
        gathered = [jnp.zeros((ROWS, LANES), jnp.float32) for _ in range(lane_groups)]
        sums = {}

        def collect(slot, value, sums=sums):
            sums[slot] = sums[slot] + value if slot in sums else value

        for c in range(tiles):
            at = p * tiles + c
            lanes = lanes_ref[at]
            got = [jnp.take_along_axis(table_ref[at, k], lanes, axis=1) for k in range(4)]
            point = [points_ref[k, at] for k in range(3)]
            pairs = [got[a] * got[b] for a, b in SYM3]
            weighted = [got[a] * got[3] for a in range(3)]
            for q, (a, b) in enumerate(SYM4):
                if a == 3:
                    values = pairs
                else:
                    factor = point[a] if b == 3 else point[a] * point[b]
                    values = [factor * pair for pair in pairs]
                for e, value in enumerate(values):
                    collect(moment_slot(q, e), value)
            for a in range(4):
                for k in range(3):
                    value = weighted[k] if a == 3 else point[a] * weighted[k]
                    collect(mixed_slot(a, k), value)
        for slot, value in sums.items():
            total = jnp.sum(value, axis=1, keepdims=True)
            g, off = divmod(slot * edges, LANES)
            gathered[g] = jnp.where(place == off, total, gathered[g])
        for n in range(pack):
            s = p * pack + n
            flat = [
                jnp.sum(part[n * edges : (n + 1) * edges], axis=0, keepdims=True) * scale
                for part in gathered
            ]
            for g in range(lane_groups):
                lines[g].append(flat[g])
    for g in range(lane_groups):
        block = jnp.concatenate(lines[g], axis=0)
        if g == lane_groups - 1:
            block = block + tail_ref[...]
        for d in range(out_ref.shape[0]):
            out_ref[d, g] = block


def sum_of(terms):
    total = None
    for term in terms:
        total = term if total is None else total + term
    return total


def product(left, right):
    return [
        [sum_of(left[a][k] * right[k][b] for k in range(3)) for b in range(3)] for a in range(3)
    ]


def transposed(matrix):
    return [[matrix[b][a] for b in range(3)] for a in range(3)]


def applied(matrix, vector):
    return [sum_of(matrix[a][k] * vector[k] for k in range(3)) for a in range(3)]


def cross(left, right):
    return [
        left[1] * right[2] - left[2] * right[1],
        left[2] * right[0] - left[0] * right[2],
        left[0] * right[1] - left[1] * right[0],
    ]


def rotated_sym(matrix, entries):
    half = product(matrix, [[entries[at3(m, k)] for k in range(3)] for m in range(3)])
    return [sum_of(half[a][k] * matrix[b][k] for k in range(3)) for a, b in SYM3]


NEXT = [(1, 2), (2, 0), (0, 1)]


def edge_terms(pair_of, own, far, swap):
    turn = [[far[3 * a + k] for k in range(3)] for a in range(3)]
    here = [[own[3 * a + k] for k in range(3)] for a in range(3)]
    start = own[9:12]
    back = transposed(turn)
    relative = product(back, here)
    shift = applied(back, [far[9 + a] - start[a] for a in range(3)])

    def halves(vector):
        return [vector, swap(vector)]

    mm = []
    xmm = [[] for _ in range(3)]
    xxmm = [[] for _ in range(6)]
    for e in range(0, len(SYM3), 2):
        moment = [pair_of(moment_slot(q, e)) for q in range(len(SYM4))]
        mm += halves(moment[at4(3, 3)])
        for a, part in enumerate(applied(relative, [moment[at4(k, 3)] for k in range(3)])):
            xmm[a] += halves(part)
        square = rotated_sym(relative, [moment[at4(a, b)] for a, b in SYM3])
        for n, part in enumerate(square):
            xxmm[n] += halves(part)
    mw = []
    xmw = [[] for _ in range(3)]
    for c in (0, 2):
        moment = [pair_of(mixed_slot(a, c)) for a in range(4)]
        mw += halves(moment[3])
        for a, part in enumerate(applied(relative, moment[:3])):
            xmw[a] += halves(part)

    def xm(a, c, d):
        return xmm[a][at3(c, d)]

    def xx(a, b, c, d):
        return xxmm[at3(a, b)][at3(c, d)]

    upper = []
    for i, i2 in SYM3:
        (j, k), (j2, k2) = NEXT[i], NEXT[i2]
        upper.append(xx(j, j2, k, k2) - xx(j, k2, k, j2) - xx(k, j2, j, k2) + xx(k, k2, j, j2))
    mixed = [[xm(j, k, d) - xm(k, j, d) for d in range(3)] for j, k in NEXT]
    lower = mm
    slope_upper = []
    for i, (j, k) in enumerate(NEXT):
        value = xmw[j][k] - xmw[k][j]
        value = value + sum_of(mixed[i][d] * shift[d] for d in range(3))
        slope_upper.append(value - sum_of(xx(j, d, k, d) - xx(k, d, j, d) for d in range(3)))
    slope_lower = []
    for i in range(3):
        value = mw[i] + sum_of(lower[at3(i, d)] * shift[d] for d in range(3))
        slope_lower.append(value - sum_of(xm(d, i, d) for d in range(3)))

    lower = rotated_sym(turn, lower)
    upper = rotated_sym(turn, upper)
    mixed = product(product(turn, mixed), back)
    slope_lower = applied(turn, slope_lower)
    slope_upper = applied(turn, slope_upper)
    slope_upper = [u + v for u, v in zip(slope_upper, cross(start, slope_lower))]
    turned = [cross(start, [lower[at3(k, d)] for k in range(3)]) for d in range(3)]
    moved_mixed = [[mixed[a][d] + turned[d][a] for d in range(3)] for a in range(3)]
    first = [cross(start, mixed[b]) for b in range(3)]
    second = [cross(start, moved_mixed[a]) for a in range(3)]
    block = [[None] * 6 for _ in range(6)]
    for n, (a, b) in enumerate(SYM3):
        block[a][b] = block[b][a] = upper[n] + first[b][a] + second[a][b]
        block[3 + a][3 + b] = block[3 + b][3 + a] = lower[n]
    for a in range(3):
        for d in range(3):
            block[a][3 + d] = block[3 + d][a] = moved_mixed[a][d]
    return block, slope_upper + slope_lower


def moved(pose, step):
    first, second, third = (0.5 * step[i] for i in range(3))
    length_sq = first * first + second * second + third * third
    inverse = 1.0 / (1.0 + length_sq)
    trace = 1.0 - length_sq
    turn = [
        [
            trace + 2.0 * first * first,
            2.0 * first * second - 2.0 * third,
            2.0 * first * third + 2.0 * second,
        ],
        [
            2.0 * first * second + 2.0 * third,
            trace + 2.0 * second * second,
            2.0 * second * third - 2.0 * first,
        ],
        [
            2.0 * first * third - 2.0 * second,
            2.0 * second * third + 2.0 * first,
            trace + 2.0 * third * third,
        ],
    ]
    turn = [[entry * inverse for entry in line] for line in turn]
    out = [
        sum_of(turn[a][k] * pose[3 * k + c] for k in range(3)) for a in range(3) for c in range(3)
    ]
    out += [sum_of(turn[a][k] * pose[9 + k] for k in range(3)) + step[3 + a] for a in range(3)]
    return out


def solve_body(first_ref, pose_ref, rows_ref, out_ref, moment_ref, final_ref, *, edges):
    devices, lane_groups, scan_dev, _ = rows_ref.shape
    scans = devices * scan_dev
    chunks = scans // LANES
    half = ROWS // 2
    blocks = [rows_ref[:, g].reshape(scans, LANES) for g in range(lane_groups)]
    for g in range(lane_groups):
        moment_ref[g * LANES : (g + 1) * LANES] = blocks[g].T

    def pair_of(slot):
        return moment_ref[slot * edges : slot * edges + ROWS]

    end = pair_of(END_SLOT).astype(jnp.int32)
    anchor = moment_ref[ANCHOR_SLOT * edges : ANCHOR_SLOT * edges + 1]
    g, off = divmod(END_SLOT * edges, LANES)
    down = lax.broadcasted_iota(jnp.int32, (scans, scans), 0)
    across = lax.broadcasted_iota(jnp.int32, (scans, scans), 1)
    here = jnp.where(down == across, 1.0, 0.0)
    across = across.astype(jnp.float32)
    minus = []
    plus = []
    for j in range(edges):
        there = jnp.where(blocks[g][:, off + j : off + j + 1] == across, 1.0, 0.0)
        minus.append((here - there).astype(jnp.bfloat16))
        plus.append((here + there).astype(jnp.bfloat16))
    minus = jnp.concatenate(minus, axis=0)
    plus = jnp.concatenate(plus, axis=0)
    upper = lax.broadcasted_iota(jnp.int32, (ROWS, scans), 0) < edges

    def swap(vector):
        return jnp.concatenate([vector[half:], vector[:half]], axis=0)

    def wide(line):
        return jnp.broadcast_to(line, (ROWS, scans))

    def at_end(table):
        parts = []
        for o in range(chunks):
            index = end[:, o * LANES : (o + 1) * LANES]
            found = None
            for q in range(chunks):
                value = jnp.take_along_axis(
                    table[:, q * LANES : (q + 1) * LANES], index & (LANES - 1), axis=1
                )
                found = value if found is None else jnp.where(lax.shift_right_logical(index, LANE_BITS) == q, value, found)
            parts.append(found)
        return parts[0] if chunks == 1 else jnp.concatenate(parts, axis=1)

    def to_scans(planes, matrix):
        empty = jnp.zeros((ROWS - len(planes), scans), jnp.float32)
        full = jnp.concatenate(
            [
                jnp.concatenate([plane[j : j + 1] for plane in planes] + [empty], axis=0)
                for j in range(edges)
            ],
            axis=1,
        )
        high = full.astype(jnp.bfloat16).astype(jnp.float32)
        rest = full - high
        middle = rest.astype(jnp.bfloat16).astype(jnp.float32)
        pieces = jnp.concatenate([high, middle, rest - middle], axis=0).astype(jnp.bfloat16)
        out = jnp.dot(pieces, matrix, preferred_element_type=jnp.float32)
        return out[:ROWS] + out[ROWS : 2 * ROWS] + out[2 * ROWS :]

    def full_sum(value):
        return jnp.sum(jnp.sum(value, axis=1, keepdims=True), axis=0, keepdims=True)

    pose = [pose_ref[i : i + 1, :] for i in range(12)]
    for _ in range(GN_ITERS):
        own = [wide(line) for line in pose]
        block, slopes = edge_terms(pair_of, own, [at_end(line) for line in own], swap)
        residual = to_scans(slopes, minus)
        diagonal = to_scans([block[a][a] for a in range(6)], plus) + anchor

        def pushed_by(vector, block=block):
            lines = [wide(vector[a : a + 1]) for a in range(6)]
            spread = [line - at_end(line) for line in lines]
            return spread, [sum_of(block[a][b] * spread[b] for b in range(6)) for a in range(6)]

        scaled = residual / diagonal
        direction = scaled
        energy = full_sum(residual * scaled)
        increment = jnp.zeros_like(residual)
        spread, pushed = pushed_by(direction)
        for sweep in range(CG_ITERS):
            inner = jnp.where(upper, sum_of(spread[a] * pushed[a] for a in range(6)), 0.0)
            step = energy / full_sum(inner + anchor * direction * direction)
            increment = increment + step * direction
            if sweep + 1 < CG_ITERS:
                image = to_scans(pushed, minus) + anchor * direction
                residual = residual - step * image
                scaled = residual / diagonal
                renewed = full_sum(residual * scaled)
                fresh_spread, fresh_pushed = pushed_by(scaled)
                ratio = renewed / energy
                spread = [fresh_spread[a] + ratio * spread[a] for a in range(6)]
                pushed = [fresh_pushed[a] + ratio * pushed[a] for a in range(6)]
                direction = scaled + ratio * direction
                energy = renewed
        pose = moved(pose, [increment[a : a + 1] for a in range(6)])
    final_ref[...] = jnp.concatenate(pose, axis=0).T
    out_ref[...] = final_ref[pl.ds(pl.multiple_of(first_ref[0], scan_dev), scan_dev)]


def refined(source_points, boundary, poses, anchor, edge_target, corr_tile, corr_source, corr_lane):
    scan_dev, bnd = boundary.shape[:2]
    edges, tiles = corr_tile.shape[1:]
    doms = lax.axis_size("dom")
    subs = lax.axis_size("sub")
    devices = subs * doms
    vectors = scan_dev * edges * tiles // ROWS
    lane_groups = -(-N_SLOTS * edges // LANES)

    packed = pl.pallas_call(
        pack_body,
        out_shape=pltpu.VMEM((scan_dev * bnd, 4, LANES), jnp.float32),
        in_specs=[vmem()],
        out_specs=vmem(),
        name="pack",
    )(in_vmem(boundary.transpose(0, 2, 1, 3)))
    window = window_of(packed, subs, doms)
    assert END_SLOT * edges // LANES == lane_groups - 1
    picked, lanes, which, tail = pl.pallas_call(
        functools.partial(pick_body, bnd=bnd),
        out_shape=[
            pltpu.VMEM((3, vectors, ROWS, LANES), jnp.float32),
            pltpu.VMEM((vectors, ROWS, LANES), jnp.int32),
            pltpu.VMEM((vectors * ROWS, LANES), jnp.int32),
            pltpu.VMEM((scan_dev, LANES), jnp.float32),
        ],
        in_specs=[smem(), smem(), smem(), vmem(), vmem(), vmem()],
        out_specs=[vmem()] * 4,
        scratch_shapes=[
            pltpu.VMEM(
                (scan_dev * edges // ROWS, 3 * source_points.shape[2] // LANES, ROWS, LANES),
                jnp.float32,
            ),
            pltpu.VMEM((vectors, ROWS, LANES), jnp.int32),
        ],
        name="pick",
    )(
        edge_target,
        corr_tile,
        anchor,
        source_points.transpose(1, 0, 2),
        corr_source,
        corr_lane,
    )
    rows = pl.pallas_call(
        functools.partial(moment_body, edges=edges, tiles=tiles),
        out_shape=jax.ShapeDtypeStruct((devices, lane_groups, scan_dev, LANES), jnp.float32),
        in_specs=[vmem()] * 5,
        out_specs=vmem(),
        scratch_shapes=[pltpu.VMEM((vectors, 4, ROWS, LANES), jnp.float32)],
        name="moments",
    )(*(in_vmem(array) for array in [which, tail, picked, lanes, window]))
    rows = lax.all_to_all(rows, AXES, 0, 0)
    first = (lax.axis_index(AXES) * scan_dev).astype(jnp.int32).reshape(1)
    return pl.pallas_call(
        functools.partial(solve_body, edges=edges),
        out_shape=jax.ShapeDtypeStruct((scan_dev, 12), jnp.float32),
        in_specs=[smem(), vmem(), vmem()],
        out_specs=vmem(),
        scratch_shapes=[
            pltpu.VMEM((lane_groups * LANES, devices * scan_dev), jnp.float32),
            pltpu.VMEM((devices * scan_dev, 12), jnp.float32),
        ],
        name="solve",
    )(first, in_vmem(poses), in_vmem(rows)).T


def solution(mesh):
    in_specs = (
        P(AXES, None, None),
        P(AXES, None, None, None),
        P(),
        P(AXES),
        P(AXES, None),
        P(AXES, None, None),
        P(AXES, None, None, None),
        P(AXES, None, None, None),
    )
    out_specs = P(None, AXES)
    step = jax.shard_map(refined, mesh=mesh, in_specs=in_specs, out_specs=out_specs, check_vma=False)
    if mesh.shape["dom"] != len(PIECES):
        return step
    return step
```
